128 devices in a mesh: dp: 8 (over x, y_hi), expert: 16 (over z, y_lo, core).
Axes of the slice: x: 4, y: 4 (y_hi: 2, y_lo: 2; y = y_hi * 2 + y_lo), z: 4, core: 2. Of those that a mesh axis runs over, the one named last changes fastest.
Arguments:
- tokens: bfloat16 [16384, 4096], P(('dp', 'expert')), may hold values from -6 to 6
- cotangent: bfloat16 [16384, 4096], P(('dp', 'expert')), may hold values from -3 to 3
- expert_ids: int32 [16384, 8, 2], P(('dp', 'expert')), may hold values from 0 to 31, as said below
- slot_ids: int32 [16384, 8, 2], P(('dp', 'expert')), may hold values from 0 to 63, as said below
- route_probs: bfloat16 [16384, 8, 2], P(('dp', 'expert')), may hold values from 0.099609375 to 1
- weights_in: bfloat16 [32, 2, 1792, 512], P('expert', None, 'dp'), may hold values from -0.25 to 0.25
- weights_out: bfloat16 [32, 1792, 512], P('expert', 'dp'), may hold values from -0.125 to 0.125
Outputs:
- grad_tokens: bfloat16 [16384, 4096], P(('dp', 'expert'))
- grad_probs: float32 [16384, 8, 2], P(('dp', 'expert'))
- grad_in: bfloat16 [32, 2, 1792, 512], P('expert', None, 'dp')
- grad_out: bfloat16 [32, 1792, 512], P('expert', 'dp')
The draws below stay inside these ranges and needn't reach their ends.
Inputs may be any that keep to these rules, and one draw needn't show every extreme that they name: `expert_ids`: each sub-token names 2 different experts. On each device the experts fall into two sets of 16, and the two ids of a sub-token come one from each set. Every expert is named by exactly 64 sub-tokens of every device. `slot_ids`: for each device and expert, the sub-tokens of that device that name the expert carry distinct slot numbers at the matching position.
All inputs are finite; a program needn't handle non-finite values.
Results may differ from the reference program's by a relative error of at most 0.012.
Values may be sent and summed in bfloat16 or wider, within the bound.
No kernel may reach another device: no remote copies, remote signals or barrier semaphores. Data moves between devices by JAX's collectives and lax.ppermute only.
A program may use at most 192 MiB of HBM per device.

```python
import jax
import jax.numpy as jnp
from jax import lax

H = 8
DS = 512
D = 4096
FF = 1792
TOP = 2
EXPERTS = 32
TOK_DEV = 128
TOKENS = 16384
CAP = 64
N_DP = 8
N_EXPERT = 16
DEVICES = 128


def route_plan(key):
    sub_count = TOK_DEV * H
    half_count = EXPERTS // 2
    pool_size = half_count * CAP
    forced = jax.random.randint(jax.random.fold_in(key, 7), (), 0, EXPERTS)
    positions = jnp.arange(pool_size, dtype=jnp.int32)

    def one_device(device_index):
        device_key = jax.random.fold_in(jax.random.fold_in(key, 13), device_index)
        shuffled = jax.random.permutation(jax.random.fold_in(device_key, 1), EXPERTS)
        picked = []
        for which_half in range(2):
            members = shuffled[which_half * half_count:(which_half + 1) * half_count]
            owners = members[positions // CAP]
            scores = jax.random.randint(jax.random.fold_in(device_key, 2 + which_half), (pool_size,), 0, 2 ** 19) * pool_size + positions
            scores = jnp.where(owners == forced, scores - 2 ** 19 * pool_size, scores)
            chosen = jnp.argsort(scores)[:sub_count]
            chosen = chosen[jax.random.permutation(jax.random.fold_in(device_key, 4 + which_half), sub_count)]
            picked.append((owners[chosen], chosen % CAP))
        swapped = jax.random.randint(jax.random.fold_in(device_key, 6), (sub_count,), 0, 2)
        first_expert = jnp.where(swapped == 1, picked[1][0], picked[0][0])
        second_expert = jnp.where(swapped == 1, picked[0][0], picked[1][0])
        first_slot = jnp.where(swapped == 1, picked[1][1], picked[0][1])
        second_slot = jnp.where(swapped == 1, picked[0][1], picked[1][1])
        expert_table = jnp.stack([first_expert, second_expert], axis=1)
        slot_table = jnp.stack([first_slot, second_slot], axis=1)
        return (expert_table, slot_table)
    expert_table, slot_table = jax.vmap(one_device)(jnp.arange(DEVICES, dtype=jnp.int32))
    return (expert_table.reshape(TOKENS, H, TOP).astype(jnp.int32), slot_table.reshape(TOKENS, H, TOP).astype(jnp.int32))


def draw_expert_ids(key, part):
    return route_plan(key)[0]


def draw_slot_ids(key, part):
    return route_plan(key)[1]


def shard_levels(rng, shape, split, low, largest):
    def one(dim, blocks):
        heights = jax.random.uniform(jax.random.fold_in(jax.random.fold_in(rng, 6), dim), (blocks,), jnp.float32, low / len(split), largest / len(split))
        return jnp.repeat(jnp.exp(heights), shape[dim] // blocks).reshape((-1,) + (1,) * (len(shape) - dim - 1))

    factor_of = one(*split[0])
    for cut in split[1:]:
        factor_of = factor_of * one(*cut)
    return factor_of


def gaussian(stream_key, shape, deviation, limit, split=(), kind=jnp.bfloat16):
    gain = shard_levels(stream_key, shape, split, -0.22, 0.18) if split else 1.0
    drawn = jax.random.normal(stream_key, shape, jnp.float32) * deviation * gain
    return jnp.minimum(jnp.maximum(drawn, -limit), limit).astype(kind)


def setup_inputs(seed: int = 0) -> dict:
    arg_keys = jax.random.split(jax.random.key(seed), 8)
    return {
        "tokens": gaussian(arg_keys[0], (TOKENS, D), 1.0, 6.0, ((0, 128),)),
        "cotangent": gaussian(arg_keys[1], (TOKENS, D), 0.5, 3.0, ((0, 128),)),
        "expert_ids": draw_expert_ids(jax.random.fold_in(arg_keys[7], 71), 0),
        "slot_ids": draw_slot_ids(jax.random.fold_in(arg_keys[7], 71), 0),
        "route_probs": jnp.clip(0.099609375 + 0.9003906 * jax.random.uniform(arg_keys[4], (TOKENS, H, TOP), jnp.float32) ** shard_levels(arg_keys[4], (TOKENS, H, TOP), ((0, 128),), -0.2, 0.2), 0.099609375, 1.0).astype(jnp.bfloat16),
        "weights_in": gaussian(arg_keys[5], (EXPERTS, 2, FF, DS), DS ** -0.5, 0.25, ((0, 16), (2, 8))),
        "weights_out": gaussian(arg_keys[6], (EXPERTS, FF, DS), FF ** -0.5, 0.125, ((0, 16), (1, 8))),
    }


def contract_last(former, latter):
    return lax.dot_general(former, latter, (((1,), (1,)), ((), ())), preferred_element_type=jnp.float32)


def expert_backward(inputs, cotangent, weighting, gate_up, down_proj):
    gate_pre = contract_last(inputs, gate_up[0])
    up_pre = contract_last(inputs, gate_up[1])
    sigmoids = jax.nn.sigmoid(gate_pre)
    activated = gate_pre * sigmoids
    hidden = (activated * up_pre).astype(jnp.bfloat16)
    output = jnp.dot(hidden, down_proj, preferred_element_type=jnp.float32)
    router_grad = jnp.sum(output * cotangent.astype(jnp.float32), axis=1).astype(jnp.bfloat16)
    scaled = (weighting.astype(jnp.float32)[:, None] * cotangent.astype(jnp.float32)).astype(jnp.bfloat16)
    dhidden = contract_last(scaled, down_proj)
    gate_grad = (dhidden * up_pre * sigmoids * (1.0 + gate_pre * (1.0 - sigmoids))).astype(jnp.bfloat16)
    up_grad = (dhidden * activated).astype(jnp.bfloat16)
    input_grad = jnp.dot(gate_grad, gate_up[0], preferred_element_type=jnp.float32)
    input_grad = (input_grad + jnp.dot(up_grad, gate_up[1], preferred_element_type=jnp.float32)).astype(jnp.bfloat16)
    return input_grad, router_grad, gate_grad, up_grad, hidden, scaled


def group_sum(left_rows, grouped):
    left_wide = left_rows.reshape(N_DP, N_EXPERT * CAP, left_rows.shape[1]).astype(jnp.float32)
    partial_sums = jnp.einsum("qrf,qrd->qfd", left_wide, grouped, precision=lax.Precision.HIGHEST)
    rounded = lax.optimization_barrier(partial_sums.astype(jnp.bfloat16))
    return jnp.sum(rounded.astype(jnp.float32), axis=0)


def reference(tokens, cotangent, expert_ids, slot_ids, route_probs, weights_in, weights_out):
    sub_count = TOKENS * H
    buffer_rows = EXPERTS * DEVICES * CAP
    device_of = (jnp.arange(sub_count, dtype=jnp.int32) // (TOK_DEV * H)).astype(jnp.int32)
    placed = expert_ids.reshape(sub_count, TOP).astype(jnp.int32) * (DEVICES * CAP) + device_of[:, None] * CAP + slot_ids.reshape(sub_count, TOP).astype(jnp.int32)
    flat_place = placed.reshape(-1).astype(jnp.int32)

    def spread(values):
        doubled = jnp.broadcast_to(values[:, None, :], (sub_count, TOP, DS)).reshape(sub_count * TOP, DS)
        filled = jnp.zeros((buffer_rows, DS), values.dtype).at[flat_place].set(doubled)
        return filled.reshape(EXPERTS, DEVICES * CAP, DS)

    input_buffer = spread(tokens.reshape(sub_count, DS))
    cotangent_buffer = spread(cotangent.reshape(sub_count, DS))
    prob_buffer = jnp.zeros((buffer_rows,), route_probs.dtype).at[flat_place].set(route_probs.reshape(-1))
    prob_buffer = prob_buffer.reshape(EXPERTS, DEVICES * CAP)

    def one_expert(packed):
        rows_in, rows_cot, rows_prob, gate_up, down_proj = packed
        input_grad, router_grad, gate_grad, up_grad, hidden, scaled = expert_backward(rows_in, rows_cot, rows_prob, gate_up, down_proj)
        grouped = rows_in.reshape(N_DP, N_EXPERT * CAP, DS).astype(jnp.float32)
        gate_sum = group_sum(gate_grad, grouped)
        up_sum = group_sum(up_grad, grouped)
        down_sum = group_sum(hidden, scaled.reshape(N_DP, N_EXPERT * CAP, DS).astype(jnp.float32))
        pair_sum = jnp.stack([gate_sum, up_sum]).astype(jnp.bfloat16)
        return input_grad, router_grad, pair_sum, down_sum.astype(jnp.bfloat16)

    input_grads, router_grads, grad_in, grad_out = lax.map(one_expert, (input_buffer, cotangent_buffer, prob_buffer, weights_in, weights_out))
    back_rows = input_grads.reshape(buffer_rows, DS)[flat_place].reshape(sub_count, TOP, DS).astype(jnp.float32)
    grad_tokens = jnp.sum(back_rows, axis=1).astype(jnp.bfloat16).reshape(TOKENS, D)
    grad_probs = router_grads.reshape(buffer_rows)[flat_place].reshape(TOKENS, H, TOP).astype(jnp.float32)
    return grad_tokens, grad_probs, grad_in, grad_out
```

```python
import functools

import jax
import jax.numpy as jnp
from jax import lax
from jax.experimental import pallas as pl
from jax.experimental.pallas import tpu as pltpu
from jax.sharding import Mesh
from jax.sharding import PartitionSpec as P

H = 8
DS = 512
CAP = 64
HALF = 32
PEERS = 32
ROWS = PEERS * HALF
SUBS = 1024
EXTRA = 8
SH = 224
F32 = jnp.float32
BF = jnp.bfloat16
AXES = ("x", "yh", "z", "yl", "core")
PLANE = ("yh", "z", "yl", "core")
VMEM = 56 * 2**20


def contract(a, b, ca, cb):
    return lax.dot_general(a, b, (((ca,), (cb,)), ((), ())), preferred_element_type=F32)


def params(mib=40):
    return pltpu.CompilerParams(vmem_limit_bytes=mib * 2**20)


def dispatch_kernel(table, tok, cot, out, *, half):
    x = jnp.concatenate([tok[:, h * DS : (h + 1) * DS] for h in range(H)], axis=0)
    c = jnp.concatenate([cot[:, h * DS : (h + 1) * DS] for h in range(H)], axis=0)
    code0 = table[0:1, :].astype(jnp.int32)
    code1 = table[1:2, :].astype(jnp.int32)
    prob0 = table[2:3, :]
    prob1 = table[3:4, :]
    block = 256
    for b in range(ROWS // block):
        row = lax.broadcasted_iota(jnp.int32, (block, SUBS), 0) + (half * ROWS + b * block)
        hit0 = row == code0
        hit1 = row == code1
        scale = jnp.where(hit0, prob0, jnp.where(hit1, prob1, 0.0)).astype(BF)
        pick = jnp.where(hit0 | hit1, 1.0, 0.0).astype(BF)
        n = block // HALF
        rows_x = contract(pick, x, 1, 0).astype(BF)
        rows_s = contract(scale, c, 1, 0).astype(BF)
        out[b * n : (b + 1) * n, 0:HALF, :] = rows_x.reshape(n, HALF, DS)
        out[b * n : (b + 1) * n, HALF : 2 * HALF, :] = rows_s.reshape(n, HALF, DS)


def dispatch(table, tok, cot, half):
    return pl.pallas_call(
        functools.partial(dispatch_kernel, half=half),
        out_shape=jax.ShapeDtypeStruct((PEERS, 2 * HALF, DS), BF),
        compiler_params=params(),
        name=f"dispatch{half}",
    )(table, tok, cot)


def expert_block(z, wg, wu, wo):
    hidden = wg.shape[0]
    x = z[:, 0:HALF, :].reshape(ROWS, DS)
    s = z[:, HALF : 2 * HALF, :].reshape(ROWS, DS)
    g = contract(wg, x, 1, 1)
    u = contract(wu, x, 1, 1)
    dh = contract(wo, s, 1, 1)
    sig = 0.5 * jnp.tanh(0.5 * g) + 0.5
    act = g * sig
    hid = (act * u).astype(BF)
    dhu = dh * u
    du = (dh * act).astype(BF)
    dg = (dhu * (sig + act * (1.0 - sig))).astype(BF)
    router = jnp.sum((dhu * act).reshape(hidden // 8, 8, ROWS), axis=0)
    dw = (contract(dg, x, 1, 0), contract(du, x, 1, 0), contract(hid, s, 1, 0))
    dx = contract(dg, wg, 0, 0) + contract(du, wu, 0, 0)
    return dw, dx, router


def first_kernel(z, *refs):
    weights, (dw, dxo, router, wbuf, acc) = refs[:8], refs[8:]
    j = pl.program_id(0)

    @pl.when(j == 0)
    def _():
        for k in range(8):
            wbuf[:, k * SH : (k + 1) * SH, :] = weights[k][...]
        acc[...] = jnp.zeros_like(acc)
        router[...] = jnp.zeros_like(router)

    here = pl.ds(pl.multiple_of(j * 2 * SH, 2 * SH), 2 * SH)
    parts, dx, r = expert_block(z, wbuf[0, here, :], wbuf[1, here, :], wbuf[2, here, :])
    for k in range(3):
        dw[k] = parts[k]
    acc[...] += dx
    router[...] += r

    @pl.when(j == 3)
    def _():
        dxo[...] = acc[...].astype(BF).reshape(PEERS, HALF, DS)


def first_half(z, weights):
    fixed3 = lambda j: (0, 0, 0)
    return pl.pallas_call(
        first_kernel,
        grid=(4,),
        in_specs=[pl.BlockSpec((PEERS, 2 * HALF, DS), fixed3)]
        + [pl.BlockSpec((3, SH, DS), fixed3)] * 8,
        out_specs=[
            pl.BlockSpec((3, 2 * SH, DS), lambda j: (0, j, 0)),
            pl.BlockSpec((PEERS, HALF, DS), fixed3),
            pl.BlockSpec((8, ROWS), lambda j: (0, 0)),
        ],
        out_shape=[
            jax.ShapeDtypeStruct((3, 8 * SH, DS), F32),
            jax.ShapeDtypeStruct((PEERS, HALF, DS), BF),
            jax.ShapeDtypeStruct((8, ROWS), F32),
        ],
        scratch_shapes=[pltpu.VMEM((3, 8 * SH, DS), BF), pltpu.VMEM((ROWS, DS), F32)],
        compiler_params=params(56),
        name="first_half",
    )(z, *weights)


def second_kernel(*refs, pairs, begin, end):
    n = 2 * pairs
    z = refs[0]
    weights = refs[1 : 1 + n]
    before = refs[1 + n]
    pos = 2 + n
    if not begin:
        acc_in, router_in = refs[pos : pos + 2]
        pos += 2
    if end:
        router_first = refs[pos]
        pos += 1
    outs = refs[pos : pos + n]
    pos += n
    acc = None
    router = None
    for p in range(pairs):
        w = [
            jnp.concatenate([weights[2 * p][k], weights[2 * p + 1][k]], axis=0) for k in range(3)
        ]
        parts, dx, r = expert_block(z, *w)
        for k in range(3):
            total = parts[k] + before[k, p * 2 * SH : (p + 1) * 2 * SH, :]
            outs[2 * p][k] = total[:SH].astype(BF)
            outs[2 * p + 1][k] = total[SH:].astype(BF)
        if acc is None and begin:
            acc, router = dx, r
        elif acc is None:
            acc, router = acc_in[...] + dx, router_in[...] + r
        else:
            acc, router = acc + dx, router + r
    if not end:
        acc_out, router_out = refs[pos : pos + 2]
        acc_out[...] = acc
        router_out[...] = router
        return
    back = refs[pos]
    back[:, 0:HALF, :] = acc.astype(BF).reshape(PEERS, HALF, DS)
    source = lax.broadcasted_iota(jnp.int32, (PEERS, ROWS), 0)
    row = lax.broadcasted_iota(jnp.int32, (PEERS, ROWS), 1)
    slot = lax.broadcasted_iota(jnp.int32, (ROWS, 128), 0)
    lane = lax.broadcasted_iota(jnp.int32, (ROWS, 128), 1)
    table = jnp.zeros((PEERS, 128), F32)
    for half, value in ((0, router_first[...]), (1, router)):
        flat = jnp.sum(value, axis=0, keepdims=True)
        spread = jnp.where(row // HALF == source, flat, 0.0).astype(BF)
        place = jnp.where(slot % HALF + half * HALF == lane, 1.0, 0.0).astype(BF)
        table = table + contract(spread, place, 1, 0)
    back[:, HALF : HALF + EXTRA, 0:128] = jnp.broadcast_to(
        table.astype(BF)[:, None, :], (PEERS, EXTRA, 128)
    )
    back[:, HALF : HALF + EXTRA, 128:DS] = jnp.zeros((PEERS, EXTRA, DS - 128), BF)


def second_half(z, weights, before, first_block, carry=None, router_first=None):
    n = len(weights)
    end = router_first is not None
    fixed3 = lambda j: (0, 0, 0)
    fixed2 = lambda j: (0, 0)
    args = [z, *weights, before]
    in_specs = [pl.BlockSpec((PEERS, 2 * HALF, DS), fixed3)]
    in_specs += [pl.BlockSpec((3, SH, DS), fixed3)] * n
    in_specs += [pl.BlockSpec((3, n * SH, DS), lambda j: (0, first_block, 0))]
    if carry is not None:
        args += list(carry)
        in_specs += [pl.BlockSpec((ROWS, DS), fixed2), pl.BlockSpec((8, ROWS), fixed2)]
    if end:
        args += [router_first]
        in_specs += [pl.BlockSpec((8, ROWS), fixed2)]
    out_specs = [pl.BlockSpec((3, SH, DS), fixed3)] * n
    out_shape = [jax.ShapeDtypeStruct((3, SH, DS), BF)] * n
    if end:
        out_specs += [pl.BlockSpec((PEERS, HALF + EXTRA, DS), fixed3)]
        out_shape += [jax.ShapeDtypeStruct((PEERS, HALF + EXTRA, DS), BF)]
    else:
        out_specs += [pl.BlockSpec((ROWS, DS), fixed2), pl.BlockSpec((8, ROWS), fixed2)]
        out_shape += [
            jax.ShapeDtypeStruct((ROWS, DS), F32),
            jax.ShapeDtypeStruct((8, ROWS), F32),
        ]
    return pl.pallas_call(
        functools.partial(second_kernel, pairs=n // 2, begin=carry is None, end=end),
        grid=(1,),
        in_specs=in_specs,
        out_specs=out_specs,
        out_shape=out_shape,
        compiler_params=params(56),
        name=f"second_half{first_block}",
    )(*args)


def picks(code0, code1, half, start, count):
    row = lax.broadcasted_iota(jnp.int32, (count, ROWS), 1) + half * ROWS
    c0 = code0[start : start + count]
    c1 = code1[start : start + count]
    return jnp.where((row == c0) | (row == c1), 1.0, 0.0).astype(BF)


def combine_first_kernel(table, back, out):
    cols = jnp.transpose(table[...])
    code0 = cols[:, 0:1].astype(jnp.int32)
    code1 = cols[:, 1:2].astype(jnp.int32)
    rows = back[...].reshape(ROWS, DS)
    count = 256
    for b in range(SUBS // count):
        out[b * count : (b + 1) * count, :] = contract(
            picks(code0, code1, 0, b * count, count), rows, 1, 0
        )


def combine_last_kernel(table, part, back, out, probs):
    cols = jnp.transpose(table[...])
    code0 = cols[:, 0:1].astype(jnp.int32)
    code1 = cols[:, 1:2].astype(jnp.int32)
    rows = back[:, 0:HALF, :].reshape(ROWS, DS)
    count = 256
    n = count // 128
    for b in range(SUBS // count):
        got = contract(picks(code0, code1, 1, b * count, count), rows, 1, 0)
        got = (got + part[b * count : (b + 1) * count, :]).astype(BF)
        for k in range(n):
            h = b * n + k
            out[:, h * DS : (h + 1) * DS] = got[k * 128 : (k + 1) * 128]
    routers = back[:, HALF : HALF + EXTRA, 0:128].reshape(PEERS * EXTRA, 128)
    source = lax.broadcasted_iota(jnp.int32, (SUBS, PEERS * EXTRA), 1)
    lane = lax.broadcasted_iota(jnp.int32, (SUBS, 128), 1)
    found = []
    for code, prob in ((code0, cols[:, 2:3]), (code1, cols[:, 3:4])):
        peer = (code % ROWS) // HALF
        slot = code % HALF + (code // ROWS) * HALF
        pick = jnp.where(source == peer * EXTRA, 1.0, 0.0).astype(BF)
        line = contract(pick, routers, 1, 0)
        value = jnp.sum(jnp.where(lane == slot, line, 0.0), axis=1, keepdims=True)
        found.append(value / prob)
    both = jnp.where(lane == 0, found[0], jnp.where(lane == 1, found[1], 0.0))
    probs[...] = jnp.transpose(both)[0:8, :]


def combine_first(table, back):
    return pl.pallas_call(
        combine_first_kernel,
        out_shape=jax.ShapeDtypeStruct((SUBS, DS), F32),
        compiler_params=params(),
        name="combine_first",
    )(table, back)


def combine_last(table, part, back):
    return pl.pallas_call(
        combine_last_kernel,
        out_shape=[
            jax.ShapeDtypeStruct((SUBS // H, H * DS), BF),
            jax.ShapeDtypeStruct((8, SUBS), F32),
        ],
        compiler_params=params(),
        name="combine_last",
    )(table, part, back)


def ring(a, step):
    return lax.ppermute(a, "x", [(i, (i + step) % 4) for i in range(4)])


def swap(a):
    return lax.ppermute(a, "yh", [(0, 1), (1, 0)])


def exchange(a):
    return lax.all_to_all(a, PLANE, 0, 0, tiled=True)


def body(tokens, cotangent, expert_ids, slot_ids, route_probs, weights_in, weights_out):
    yh = lax.axis_index("yh")
    both = jnp.concatenate([weights_in, weights_out[:, None]], axis=1)
    mine = jnp.where(yh == 0, both[0], both[1])
    theirs = jnp.where(yh == 0, both[1], both[0])
    w_p = swap(theirs)
    w_o = mine
    w_o_m = ring(w_o, 1)
    w_o_p = ring(w_o, -1)
    w_p_m = ring(w_p, 1)
    w_p_p = ring(w_p, -1)
    w_o_2 = ring(w_o_m, 1)
    w_p_2 = ring(w_p_p, -1)

    dest = expert_ids % 2 * (PEERS // 2) + expert_ids // 2
    code = slot_ids // HALF * ROWS + dest * HALF + slot_ids % HALF
    table = jnp.concatenate([code.astype(F32), route_probs.astype(F32)], axis=2)
    table = jnp.transpose(table, (2, 1, 0)).reshape(4, SUBS)
    table = jnp.pad(table, ((0, 4), (0, 0)))

    z1 = exchange(dispatch(table, tokens, cotangent, 0))
    z2 = exchange(dispatch(table, tokens, cotangent, 1))

    weights = [w_o_2, w_p_2, w_o_p, w_p_p, w_o_m, w_p_m, w_o, w_p]
    dw_first, back1, router1 = first_half(z1, weights)
    back1 = exchange(back1)
    o_2, p_2, acc, router = second_half(z2, weights[0:2], dw_first, 0)
    o_2 = ring(o_2, 1)
    p_2 = ring(p_2, -1)
    o_p, p_p, acc, router = second_half(z2, weights[2:4], dw_first, 1, (acc, router))
    o_m, p_m, acc, router = second_half(z2, weights[4:6], dw_first, 2, (acc, router))
    p_p = ring(p_p, 1)
    p_m = ring((p_m.astype(F32) + p_2.astype(F32)).astype(BF), -1)
    o_m = ring(o_m, -1)
    o_p = ring((o_p.astype(F32) + o_2.astype(F32)).astype(BF), 1)
    o_0, p_0, back2 = second_half(z2, weights[6:8], dw_first, 3, (acc, router), router1)
    back2 = exchange(back2)

    p_sum = (p_0.astype(F32) + p_p.astype(F32) + p_m.astype(F32)).astype(BF)
    other = swap(p_sum)
    own = (o_0.astype(F32) + o_p.astype(F32) + o_m.astype(F32)).astype(BF)
    low = jnp.where(yh == 0, own, other)
    high = jnp.where(yh == 0, other, own)
    grad_in = jnp.stack([low[0:2], high[0:2]])
    grad_out = jnp.stack([low[2], high[2]])

    part = combine_first(table, back1)
    grad_tokens, probs = combine_last(table, part, back2)
    grad_probs = jnp.transpose(probs[0:2].reshape(2, H, SUBS // H), (2, 1, 0))
    return grad_tokens, grad_probs, grad_in, grad_out


def solution(mesh):
    wide = Mesh(mesh.devices.reshape(4, 2, 4, 2, 2), AXES)
    dp = ("x", "yh")
    expert = ("z", "yl", "core")
    rows2 = P(AXES, None)
    rows3 = P(AXES, None, None)
    w_in = P(expert, None, dp, None)
    w_out = P(expert, dp, None)
    return jax.shard_map(
        body,
        mesh=wide,
        in_specs=(rows2, rows2, rows3, rows3, rows3, w_in, w_out),
        out_specs=(rows2, rows3, w_in, w_out),
        check_vma=False,
    )
```

```python
import functools

import jax
import jax.numpy as jnp
from jax import lax
from jax.experimental import pallas as pl
from jax.experimental.pallas import tpu as pltpu
from jax.sharding import Mesh
from jax.sharding import PartitionSpec as P

H = 8
DS = 512
PEERS = 32
SLOTS = (40, 24)
GROUP = 8
SUBS = 1024
EXTRA = 8
SH = 224
F32 = jnp.float32
BF = jnp.bfloat16
AXES = ("x", "yh", "z", "yl", "core")
PLANE = ("yh", "z", "yl", "core")


def contract(a, b, ca, cb):
    return lax.dot_general(a, b, (((ca,), (cb,)), ((), ())), preferred_element_type=F32)


def in_hbm(a):
    return pltpu.with_memory_space_constraint(a, pltpu.HBM)


def params(mib=24):
    return pltpu.CompilerParams(vmem_limit_bytes=mib * 2**20)


def dispatch_kernel(table, tok, cot, out, *, part):
    slots = SLOTS[part]
    base = part * PEERS * SLOTS[0]
    x = jnp.concatenate([tok[:, h * DS : (h + 1) * DS] for h in range(H)], axis=0)
    c = jnp.concatenate([cot[:, h * DS : (h + 1) * DS] for h in range(H)], axis=0)
    code0 = table[0:1, :].astype(jnp.int32)
    code1 = table[1:2, :].astype(jnp.int32)
    prob0 = table[2:3, :]
    prob1 = table[3:4, :]
    block = GROUP * slots
    row = lax.broadcasted_iota(jnp.int32, (block, SUBS), 0) + (base + pl.program_id(0) * block)
    hit0 = row == code0
    hit1 = row == code1
    scale = jnp.where(hit0, prob0, jnp.where(hit1, prob1, 0.0)).astype(BF)
    pick = jnp.where(hit0 | hit1, 1.0, 0.0).astype(BF)
    out[:, 0:slots, :] = contract(pick, x, 1, 0).astype(BF).reshape(GROUP, slots, DS)
    out[:, slots : 2 * slots, :] = contract(scale, c, 1, 0).astype(BF).reshape(GROUP, slots, DS)


def dispatch(table, tok, cot, part):
    slots = SLOTS[part]
    fixed = lambda b: (0, 0)
    return pl.pallas_call(
        functools.partial(dispatch_kernel, part=part),
        grid=(PEERS // GROUP,),
        in_specs=[
            pl.BlockSpec((8, SUBS), fixed),
            pl.BlockSpec((SUBS // H, H * DS), fixed),
            pl.BlockSpec((SUBS // H, H * DS), fixed),
        ],
        out_specs=pl.BlockSpec((GROUP, 2 * slots, DS), lambda b: (b, 0, 0)),
        out_shape=pltpu.HBM((PEERS, 2 * slots, DS), BF),
        compiler_params=params(),
    )(table, tok, cot)


def expert_block(z, slots, wg, wu, wo):
    hidden = wg.shape[0]
    rows = PEERS * slots
    x = z[:, 0:slots, :].reshape(rows, DS)
    s = z[:, slots : 2 * slots, :].reshape(rows, DS)
    g = contract(wg, x, 1, 1)
    u = contract(wu, x, 1, 1)
    dh = contract(wo, s, 1, 1)
    sig = 0.5 * jnp.tanh(0.5 * g) + 0.5
    act = g * sig
    hid = (act * u).astype(BF)
    dhu = dh * u
    du = (dh * act).astype(BF)
    dg = (dhu * (sig + act * (1.0 - sig))).astype(BF)
    router = jnp.sum((dhu * act).reshape(hidden // 8, 8, rows), axis=0)
    dw = (contract(dg, x, 1, 0), contract(du, x, 1, 0), contract(hid, s, 1, 0))
    dx = contract(dg, wg, 0, 0) + contract(du, wu, 0, 0)
    return dw, dx, router


HBM = pl.BlockSpec(memory_space=pltpu.HBM)
WHOLE = pl.BlockSpec(memory_space=pltpu.VMEM)


def first_kernel(z_in, *refs):
    weights, (dw, dxo, router, z, wbuf, acc, stage, zsem, wsem, osem) = refs[:8], refs[8:]
    rows_in = pltpu.make_async_copy(z_in, z, zsem)
    rows_in.start()

    def fetch(k, slot):
        here = pl.ds(pl.multiple_of(slot * SH, SH), SH)
        return pltpu.make_async_copy(weights[k], wbuf.at[:, here, :], wsem.at[slot])

    def flush(j, slot):
        here = pl.ds(pl.multiple_of(j * 2 * SH, 2 * SH), 2 * SH)
        return pltpu.make_async_copy(stage.at[slot], dw.at[:, here, :], osem.at[slot])

    for k in range(8):
        fetch(k, k).start()
    acc[...] = jnp.zeros_like(acc)
    router[...] = jnp.zeros_like(router)
    rows_in.wait()

    def block(j, carry):
        fetch(0, 2 * j).wait()
        fetch(1, 2 * j + 1).wait()
        here = pl.ds(pl.multiple_of(j * 2 * SH, 2 * SH), 2 * SH)
        parts, dx, r = expert_block(
            z, SLOTS[0], wbuf[0, here, :], wbuf[1, here, :], wbuf[2, here, :]
        )
        slot = j % 2

        @pl.when(j >= 2)
        def _():
            flush(j - 2, slot).wait()

        for k in range(3):
            stage[slot, k] = parts[k]
        acc[...] += dx
        router[...] += r
        flush(j, slot).start()
        return carry

    lax.fori_loop(0, 4, block, 0)
    dxo[...] = acc[...].astype(BF).reshape(PEERS, SLOTS[0], DS)
    flush(2, 0).wait()
    flush(3, 1).wait()


def first_part(z, weights):
    rows = PEERS * SLOTS[0]
    return pl.pallas_call(
        first_kernel,
        in_specs=[HBM] * 9,
        out_specs=[HBM, WHOLE, WHOLE],
        out_shape=[
            pltpu.HBM((3, 8 * SH, DS), F32),
            pltpu.HBM((PEERS, SLOTS[0], DS), BF),
            jax.ShapeDtypeStruct((8, rows), F32),
        ],
        scratch_shapes=[
            pltpu.VMEM((PEERS, 2 * SLOTS[0], DS), BF),
            pltpu.VMEM((3, 8 * SH, DS), BF),
            pltpu.VMEM((rows, DS), F32),
            pltpu.VMEM((2, 3, 2 * SH, DS), F32),
            pltpu.SemaphoreType.DMA,
            pltpu.SemaphoreType.DMA((8,)),
            pltpu.SemaphoreType.DMA((2,)),
        ],
        compiler_params=params(40),
        name="first_part",
    )(*[in_hbm(a) for a in (z, *weights)])


def second_kernel(*refs, pairs, first, begin, end):
    n = 2 * pairs
    slots = SLOTS[1]
    z = refs[0]
    weights = refs[1 : 1 + n]
    before = refs[1 + n]
    pos = 2 + n
    if not begin:
        acc_in, router_in = refs[pos : pos + 2]
        pos += 2
    if end:
        router_first = refs[pos]
        pos += 1
    outs = refs[pos : pos + n]
    pos += n
    if end:
        back, router, acc, wbuf, stage, obuf, asem, wsem, bsem, ssem = refs[pos:]
    else:
        acc_out, router, acc, wbuf, stage, obuf, asem, wsem, bsem, ssem = refs[pos:]

    def fetch(k, slot):
        half = k % 2
        return pltpu.make_async_copy(
            weights[k], wbuf.at[slot, :, half * SH : (half + 1) * SH, :], wsem.at[slot, half]
        )

    def load(p):
        here = pl.ds(pl.multiple_of((first + p) * 2 * SH, 2 * SH), 2 * SH)
        return pltpu.make_async_copy(before.at[:, here, :], stage.at[p], bsem.at[p])

    def store(p, half):
        return pltpu.make_async_copy(
            obuf.at[p, :, half * SH : (half + 1) * SH, :], outs[2 * p + half], ssem.at[p, half]
        )

    for k in range(n):
        fetch(k, k // 2).start()
    for p in range(pairs):
        load(p).start()
    if begin:
        router[...] = jnp.zeros_like(router)
        acc[...] = jnp.zeros_like(acc)
    else:
        acc_load = pltpu.make_async_copy(acc_in, acc, asem)
        acc_load.start()
        router[...] = router_in[...]

    def block(p, carry):
        fetch(0, p).wait()
        fetch(1, p).wait()
        parts, dx, r = expert_block(z, slots, wbuf[p, 0], wbuf[p, 1], wbuf[p, 2])
        load(p).wait()
        for k in range(3):
            obuf[p, k] = (parts[k] + stage[p, k]).astype(BF)
        for q in range(pairs):

            @pl.when(p == q)
            def _():
                for half in range(2):
                    store(q, half).start()

        if not begin:

            @pl.when(p == 0)
            def _():
                acc_load.wait()

        acc[...] += dx
        router[...] += r
        return carry

    if pairs == 1:
        block(0, 0)
    else:
        lax.fori_loop(0, pairs, block, 0)

    def drain():
        for p in range(pairs):
            for half in range(2):
                store(p, half).wait()

    if not end:
        acc_save = pltpu.make_async_copy(acc, acc_out, asem)
        acc_save.start()
        drain()
        acc_save.wait()
        return
    back[:, 0:slots, :] = acc[...].astype(BF).reshape(PEERS, slots, DS)
    table = jnp.zeros((PEERS, 128), F32)
    for part, value in ((0, router_first[...]), (1, router[...])):
        count = SLOTS[part]
        total = PEERS * count
        source = lax.broadcasted_iota(jnp.int32, (PEERS, total), 0) * count
        row = lax.broadcasted_iota(jnp.int32, (PEERS, total), 1)
        flat = jnp.sum(value, axis=0, keepdims=True)
        spread = jnp.where((row >= source) & (row < source + count), flat, 0.0).astype(BF)
        slot = lax.broadcasted_iota(jnp.int32, (total, 128), 0) % count + part * SLOTS[0]
        lane = lax.broadcasted_iota(jnp.int32, (total, 128), 1)
        place = jnp.where(slot == lane, 1.0, 0.0).astype(BF)
        table = table + contract(spread, place, 1, 0)
    back[:, slots : slots + EXTRA, 0:128] = jnp.broadcast_to(
        table.astype(BF)[:, None, :], (PEERS, EXTRA, 128)
    )
    back[:, slots : slots + EXTRA, 128:DS] = jnp.zeros((PEERS, EXTRA, DS - 128), BF)
    drain()


def second_part(z, weights, before, first, carry=None, router_first=None):
    n = len(weights)
    end = router_first is not None
    rows = PEERS * SLOTS[1]
    args = [z, *[in_hbm(a) for a in (*weights, before)]]
    in_specs = [WHOLE] + [HBM] * (n + 1)
    if carry is not None:
        args += [in_hbm(carry[0]), carry[1]]
        in_specs += [HBM, WHOLE]
    if end:
        args += [router_first]
        in_specs += [WHOLE]
    out_shape = [pltpu.HBM((3, SH, DS), BF)] * n
    scratch = []
    if end:
        out_shape += [pltpu.HBM((PEERS, SLOTS[1] + EXTRA, DS), BF)]
        scratch += [pltpu.VMEM((8, rows), F32)]
        out_specs = [HBM] * n + [WHOLE]
    else:
        out_shape += [pltpu.HBM((rows, DS), F32), jax.ShapeDtypeStruct((8, rows), F32)]
        out_specs = [HBM] * (n + 1) + [WHOLE]
    scratch += [pltpu.VMEM((rows, DS), F32)]
    scratch += [
        pltpu.VMEM((n // 2, 3, 2 * SH, DS), BF),
        pltpu.VMEM((n // 2, 3, 2 * SH, DS), F32),
        pltpu.VMEM((n // 2, 3, 2 * SH, DS), BF),
        pltpu.SemaphoreType.DMA,
        pltpu.SemaphoreType.DMA((n // 2, 2)),
        pltpu.SemaphoreType.DMA((n // 2,)),
        pltpu.SemaphoreType.DMA((n // 2, 2)),
    ]
    return pl.pallas_call(
        functools.partial(
            second_kernel, pairs=n // 2, first=first, begin=carry is None, end=end
        ),
        in_specs=in_specs,
        out_specs=out_specs,
        out_shape=out_shape,
        scratch_shapes=scratch,
        compiler_params=params(30),
    )(*args)


def picks(codes, part, start, count):
    rows = PEERS * SLOTS[part]
    row = lax.broadcasted_iota(jnp.int32, (count, rows), 1) + part * PEERS * SLOTS[0]
    code0, code1 = (c[start : start + count] for c in codes)
    return jnp.where((row == code0) | (row == code1), 1.0, 0.0).astype(BF)


def columns(table):
    cols = jnp.transpose(table[...])
    whole = lambda k: cols[:, k : k + 1].astype(jnp.int32)
    return (whole(0), whole(1)), (cols[:, 2:3], cols[:, 3:4]), (whole(4), whole(5)), (whole(6), whole(7))


def combine_first_kernel(table, back, out):
    codes = columns(table)[0]
    rows = back[...].reshape(PEERS * SLOTS[0], DS)
    count = 256
    for b in range(SUBS // count):
        out[b * count : (b + 1) * count, :] = contract(
            picks(codes, 0, b * count, count), rows, 1, 0
        )


def combine_last_kernel(table, part, back, out, probs):
    codes, weight, peer, slot = columns(table)
    rows = back[:, 0 : SLOTS[1], :].reshape(PEERS * SLOTS[1], DS)
    count = 256
    n = count // 128
    for b in range(SUBS // count):
        got = contract(picks(codes, 1, b * count, count), rows, 1, 0)
        got = (got + part[b * count : (b + 1) * count, :]).astype(BF)
        for k in range(n):
            h = b * n + k
            out[:, h * DS : (h + 1) * DS] = got[k * 128 : (k + 1) * 128]
    routers = back[:, SLOTS[1] : SLOTS[1] + EXTRA, 0:128].reshape(PEERS * EXTRA, 128)
    source = lax.broadcasted_iota(jnp.int32, (SUBS, PEERS * EXTRA), 1)
    lane = lax.broadcasted_iota(jnp.int32, (SUBS, 128), 1)
    found = []
    for k in range(2):
        pick = jnp.where(source == peer[k] * EXTRA, 1.0, 0.0).astype(BF)
        line = contract(pick, routers, 1, 0)
        value = jnp.sum(jnp.where(lane == slot[k], line, 0.0), axis=1, keepdims=True)
        found.append(value / weight[k])
    both = jnp.where(lane == 0, found[0], jnp.where(lane == 1, found[1], 0.0))
    probs[...] = jnp.transpose(both)[0:8, :]


def combine_first(table, back):
    return pl.pallas_call(
        combine_first_kernel,
        out_shape=jax.ShapeDtypeStruct((SUBS, DS), F32),
        compiler_params=params(),
        name="combine_first",
    )(table, back)


def combine_last(table, part, back):
    return pl.pallas_call(
        combine_last_kernel,
        out_shape=[
            jax.ShapeDtypeStruct((SUBS // H, H * DS), BF),
            jax.ShapeDtypeStruct((8, SUBS), F32),
        ],
        compiler_params=params(),
        name="combine_last",
    )(table, part, back)


def final_kernel(which, own0, own1, own2, other, grad_in, grad_out):
    a = which[0]
    b = 1 - a
    for k in range(3):
        total = own0[k].astype(F32) + own1[k].astype(F32) + own2[k].astype(F32)
        total = total.astype(BF)
        if k < 2:
            grad_in[a, k] = total
            grad_in[b, k] = other[k]
        else:
            grad_out[a] = total
            grad_out[b] = other[k]


def final(which, own, other):
    vmem = pl.BlockSpec(memory_space=pltpu.VMEM)
    return pl.pallas_call(
        final_kernel,
        in_specs=[pl.BlockSpec(memory_space=pltpu.SMEM)] + [vmem] * 4,
        out_shape=[
            jax.ShapeDtypeStruct((2, 2, SH, DS), BF),
            jax.ShapeDtypeStruct((2, SH, DS), BF),
        ],
        compiler_params=params(),
        name="final",
    )(which, *own, other)


def ring(a, step):
    return lax.ppermute(a, "x", [(i, (i + step) % 4) for i in range(4)])


def swap(a):
    return lax.ppermute(a, "yh", [(0, 1), (1, 0)])


def exchange(a):
    return lax.all_to_all(a, PLANE, 0, 0, tiled=True)


def add(*arrays):
    return sum(a.astype(F32) for a in arrays).astype(BF)


def layer(tokens, cotangent, expert_ids, slot_ids, route_probs, weights_in, weights_out):
    yh = lax.axis_index("yh")
    both = jnp.concatenate([weights_in, weights_out[:, None]], axis=1)
    theirs = jnp.where(yh == 0, both[1], both[0])
    w_o = jnp.where(yh == 0, both[0], both[1])
    w_p = swap(theirs)
    w_o_m = ring(w_o, 1)
    w_o_p = ring(w_o, -1)
    w_p_m = ring(w_p, 1)
    w_p_p = ring(w_p, -1)
    w_o_2 = ring(w_o_m, 1)
    w_p_2 = ring(w_p_p, -1)

    dest = expert_ids % 2 * (PEERS // 2) + expert_ids // 2
    code = jnp.where(
        slot_ids < SLOTS[0],
        dest * SLOTS[0] + slot_ids,
        PEERS * SLOTS[0] + dest * SLOTS[1] + slot_ids - SLOTS[0],
    )
    table = [code, route_probs, dest, slot_ids]
    table = jnp.concatenate([t.astype(F32) for t in table], axis=2)
    table = jnp.transpose(table, (2, 1, 0)).reshape(8, SUBS)

    z1 = exchange(dispatch(table, tokens, cotangent, 0))
    z2 = exchange(dispatch(table, tokens, cotangent, 1))

    weights = [w_o_2, w_p_2, w_o_p, w_p_p, w_o_m, w_p_m, w_o, w_p]
    dw_first, back1, router1 = first_part(z1, weights)
    back1 = exchange(back1)
    o_2, p_2, *carry = second_part(z2, weights[0:2], dw_first, 0)
    o_2 = ring(o_2, 1)
    p_2 = ring(p_2, -1)
    o_p, p_p, o_m, p_m, *carry = second_part(z2, weights[2:6], dw_first, 1, carry)
    p_p = ring(p_p, 1)
    p_m = ring(add(p_m, p_2), -1)
    o_p = ring(add(o_p, o_2), 1)
    o_m = ring(o_m, -1)
    o_0, p_0, back2 = second_part(z2, weights[6:8], dw_first, 3, carry, router1)
    back2 = exchange(back2)

    other = swap(add(p_0, p_p, p_m))
    grad_in, grad_out = final(yh.astype(jnp.int32).reshape(1), (o_0, o_p, o_m), other)

    part = combine_first(table, back1)
    grad_tokens, probs = combine_last(table, part, back2)
    grad_probs = jnp.transpose(probs[0:2].reshape(2, H, SUBS // H), (2, 1, 0))
    return grad_tokens, grad_probs, grad_in, grad_out


def solution(mesh):
    wide = Mesh(mesh.devices.reshape(4, 2, 4, 2, 2), AXES)
    dp = ("x", "yh")
    expert = ("z", "yl", "core")
    rows2 = P(AXES, None)
    rows3 = P(AXES, None, None)
    w_in = P(expert, None, dp, None)
    w_out = P(expert, dp, None)
    return jax.shard_map(
        layer,
        mesh=wide,
        in_specs=(rows2, rows2, rows3, rows3, rows3, w_in, w_out),
        out_specs=(rows2, rows3, w_in, w_out),
        check_vma=False,
    )
```

```python
import functools

import jax
import jax.numpy as jnp
from jax import lax
from jax.experimental import pallas as pl
from jax.experimental.pallas import tpu as pltpu
from jax.sharding import Mesh
from jax.sharding import PartitionSpec as P

H = 8
DS = 512
PEERS = 32
SLOTS = (32, 32)
GROUP = 8
SUBS = 1024
EXTRA = 8
SH = 224
F32 = jnp.float32
BF = jnp.bfloat16
AXES = ("x", "yh", "z", "yl", "core")
PLANE = ("yh", "z", "yl", "core")


def contract(a, b, ca, cb):
    return lax.dot_general(a, b, (((ca,), (cb,)), ((), ())), preferred_element_type=F32)


def in_hbm(a):
    return pltpu.with_memory_space_constraint(a, pltpu.HBM)


def params(mib=24):
    return pltpu.CompilerParams(vmem_limit_bytes=mib * 2**20)


def dispatch_kernel(table, tok, cot, out, *, part):
    slots = SLOTS[part]
    base = part * PEERS * SLOTS[0]
    x = jnp.concatenate([tok[:, h * DS : (h + 1) * DS] for h in range(H)], axis=0)
    c = jnp.concatenate([cot[:, h * DS : (h + 1) * DS] for h in range(H)], axis=0)
    code0 = table[0:1, :].astype(jnp.int32)
    code1 = table[1:2, :].astype(jnp.int32)
    prob0 = table[2:3, :]
    prob1 = table[3:4, :]
    block = GROUP * slots
    row = lax.broadcasted_iota(jnp.int32, (block, SUBS), 0) + (base + pl.program_id(0) * block)
    hit0 = row == code0
    hit1 = row == code1
    scale = jnp.where(hit0, prob0, jnp.where(hit1, prob1, 0.0)).astype(BF)
    pick = jnp.where(hit0 | hit1, 1.0, 0.0).astype(BF)
    out[:, 0:slots, :] = contract(pick, x, 1, 0).astype(BF).reshape(GROUP, slots, DS)
    out[:, slots : 2 * slots, :] = contract(scale, c, 1, 0).astype(BF).reshape(GROUP, slots, DS)


def dispatch(table, tok, cot, part):
    slots = SLOTS[part]
    fixed = lambda b: (0, 0)
    return pl.pallas_call(
        functools.partial(dispatch_kernel, part=part),
        grid=(PEERS // GROUP,),
        in_specs=[
            pl.BlockSpec((8, SUBS), fixed),
            pl.BlockSpec((SUBS // H, H * DS), fixed),
            pl.BlockSpec((SUBS // H, H * DS), fixed),
        ],
        out_specs=pl.BlockSpec((GROUP, 2 * slots, DS), lambda b: (b, 0, 0)),
        out_shape=pltpu.HBM((PEERS, 2 * slots, DS), BF),
        compiler_params=params(),
    )(table, tok, cot)


def expert_block(z, slots, wg, wu, wo):
    hidden = wg.shape[0]
    rows = PEERS * slots
    x = z[:, 0:slots, :].reshape(rows, DS)
    s = z[:, slots : 2 * slots, :].reshape(rows, DS)
    g = contract(wg, x, 1, 1)
    u = contract(wu, x, 1, 1)
    dh = contract(wo, s, 1, 1)
    sig = 0.5 * jnp.tanh(0.5 * g) + 0.5
    act = g * sig
    hid = (act * u).astype(BF)
    dhu = dh * u
    du = (dh * act).astype(BF)
    dg = (dhu * (sig + act * (1.0 - sig))).astype(BF)
    router = jnp.sum((dhu * act).reshape(hidden // 8, 8, rows), axis=0)
    dw = (contract(dg, x, 1, 0), contract(du, x, 1, 0), contract(hid, s, 1, 0))
    dx = contract(dg, wg, 0, 0) + contract(du, wu, 0, 0)
    return dw, dx, router


HBM = pl.BlockSpec(memory_space=pltpu.HBM)
WHOLE = pl.BlockSpec(memory_space=pltpu.VMEM)
UNITS = 2 * SH


def router_rows(back, slots, router_first, router):
    table = jnp.zeros((PEERS, 128), F32)
    for part, value in ((0, router_first), (1, router)):
        count = SLOTS[part]
        total = PEERS * count
        source = lax.broadcasted_iota(jnp.int32, (PEERS, total), 0) * count
        row = lax.broadcasted_iota(jnp.int32, (PEERS, total), 1)
        flat = jnp.sum(value, axis=0, keepdims=True)
        spread = jnp.where((row >= source) & (row < source + count), flat, 0.0).astype(BF)
        slot = lax.broadcasted_iota(jnp.int32, (total, 128), 0) % count + part * SLOTS[0]
        lane = lax.broadcasted_iota(jnp.int32, (total, 128), 1)
        place = jnp.where(slot == lane, 1.0, 0.0).astype(BF)
        table = table + contract(spread, place, 1, 0)
    back[:, slots : slots + EXTRA, 0:128] = jnp.broadcast_to(
        table.astype(BF)[:, None, :], (PEERS, EXTRA, 128)
    )
    back[:, slots : slots + EXTRA, 128:DS] = jnp.zeros((PEERS, EXTRA, DS - 128), BF)


def expert_kernel(*refs, part, end):
    slots = SLOTS[part]
    refs = list(refs)
    take = lambda n: [refs.pop(0) for _ in range(n)]
    (z,) = take(1)
    weights = take(4)
    before = take(1)[0] if part else None
    acc_in, router_in = take(2) if end else (None, None)
    router_first = take(1)[0] if part and end else None
    outs = take(4 if part else 1)
    (dx_out,) = take(1)
    router_out = None if part and end else take(1)[0]
    acc, wbuf, stage, obuf, asem, wsem, bsem, ssem = refs

    def units(p):
        return pl.ds(pl.multiple_of(p * UNITS, UNITS), UNITS)

    def fetch(k, slot):
        half = k % 2
        return pltpu.make_async_copy(
            weights[k], wbuf.at[slot, :, half * SH : (half + 1) * SH, :], wsem.at[slot, half]
        )

    def load(p):
        return pltpu.make_async_copy(before.at[:, units(p), :], stage.at[p], bsem.at[p])

    def store_wide(p):
        return pltpu.make_async_copy(stage.at[p], outs[0].at[:, units(p), :], bsem.at[p])

    def store(p, half):
        return pltpu.make_async_copy(
            obuf.at[p, :, half * SH : (half + 1) * SH, :], outs[2 * p + half], ssem.at[p, half]
        )

    for k in range(4):
        fetch(k, k // 2).start()
    if part:
        for p in range(2):
            load(p).start()
    if end:
        acc_load = pltpu.make_async_copy(acc_in, acc, asem)
        acc_load.start()
    else:
        acc[...] = jnp.zeros_like(acc)
    router = jnp.zeros((8, PEERS * slots), F32) if not end else router_in[...]

    def block(p, router):
        fetch(0, p).wait()
        fetch(1, p).wait()
        parts, dx, r = expert_block(z, slots, wbuf[p, 0], wbuf[p, 1], wbuf[p, 2])
        if part:
            load(p).wait()
            for k in range(3):
                obuf[p, k] = (parts[k] + stage[p, k]).astype(BF)
            for q in range(2):

                @pl.when(p == q)
                def _():
                    for half in range(2):
                        store(q, half).start()
        else:
            for k in range(3):
                stage[p, k] = parts[k]
            store_wide(p).start()
        if end:

            @pl.when(p == 0)
            def _():
                acc_load.wait()

        acc[...] += dx
        return router + r

    router = lax.fori_loop(0, 2, block, router)
    if end:
        dx_out[:, 0:slots, :] = acc[...].astype(BF).reshape(PEERS, slots, DS)
    else:
        acc_save = pltpu.make_async_copy(acc, dx_out, asem)
        acc_save.start()
    if router_out is None:
        router_rows(dx_out, slots, router_first[...], router)
    else:
        router_out[...] = router
    for p in range(2):
        if part:
            store(p, 0).wait()
            store(p, 1).wait()
        else:
            store_wide(p).wait()
    if not end:
        acc_save.wait()


def expert_part(part, z, weights, before=None, carry=None, router_first=None):
    end = carry is not None
    slots = SLOTS[part]
    rows = PEERS * slots
    args = [z, *[in_hbm(w) for w in weights]]
    in_specs = [WHOLE] + [HBM] * 4
    if part:
        args += [in_hbm(before)]
        in_specs += [HBM]
    if end:
        args += [in_hbm(carry[0]), carry[1]]
        in_specs += [HBM, WHOLE]
    if part and end:
        args += [router_first]
        in_specs += [WHOLE]
    if part:
        out_shape = [pltpu.HBM((3, SH, DS), BF)] * 4
        out_specs = [HBM] * 4
    else:
        out_shape = [pltpu.HBM((3, 4 * SH, DS), F32)]
        out_specs = [HBM]
    if end:
        out_shape += [pltpu.HBM((PEERS, slots + part * EXTRA, DS), BF)]
        out_specs += [WHOLE]
    else:
        out_shape += [pltpu.HBM((rows, DS), F32)]
        out_specs += [HBM]
    if not (part and end):
        out_shape += [jax.ShapeDtypeStruct((8, rows), F32)]
        out_specs += [WHOLE]
    return pl.pallas_call(
        functools.partial(expert_kernel, part=part, end=end),
        in_specs=in_specs,
        out_specs=out_specs,
        out_shape=out_shape,
        scratch_shapes=[
            pltpu.VMEM((rows, DS), F32),
            pltpu.VMEM((2, 3, UNITS, DS), BF),
            pltpu.VMEM((2, 3, UNITS, DS), F32),
            pltpu.VMEM((2, 3, UNITS, DS) if part else (8, 128), BF),
            pltpu.SemaphoreType.DMA,
            pltpu.SemaphoreType.DMA((2, 2)),
            pltpu.SemaphoreType.DMA((2,)),
            pltpu.SemaphoreType.DMA((2, 2)),
        ],
        compiler_params=params(36),
    )(*args)


def picks(codes, part, start, count):
    rows = PEERS * SLOTS[part]
    row = lax.broadcasted_iota(jnp.int32, (count, rows), 1) + part * PEERS * SLOTS[0]
    code0, code1 = (c[start : start + count] for c in codes)
    return jnp.where((row == code0) | (row == code1), 1.0, 0.0).astype(BF)


def columns(table):
    cols = jnp.transpose(table[...])
    whole = lambda k: cols[:, k : k + 1].astype(jnp.int32)
    return (whole(0), whole(1)), (cols[:, 2:3], cols[:, 3:4]), (whole(4), whole(5)), (whole(6), whole(7))


def combine_first_kernel(table, back, out):
    codes = columns(table)[0]
    rows = back[...].reshape(PEERS * SLOTS[0], DS)
    count = 256
    for b in range(SUBS // count):
        out[b * count : (b + 1) * count, :] = contract(
            picks(codes, 0, b * count, count), rows, 1, 0
        )


def combine_last_kernel(table, part, back, out, probs):
    codes, weight, peer, slot = columns(table)
    rows = back[:, 0 : SLOTS[1], :].reshape(PEERS * SLOTS[1], DS)
    count = 256
    n = count // 128
    for b in range(SUBS // count):
        got = contract(picks(codes, 1, b * count, count), rows, 1, 0)
        got = (got + part[b * count : (b + 1) * count, :]).astype(BF)
        for k in range(n):
            h = b * n + k
            out[:, h * DS : (h + 1) * DS] = got[k * 128 : (k + 1) * 128]
    routers = back[:, SLOTS[1] : SLOTS[1] + EXTRA, 0:128].reshape(PEERS * EXTRA, 128)
    source = lax.broadcasted_iota(jnp.int32, (SUBS, PEERS * EXTRA), 1)
    lane = lax.broadcasted_iota(jnp.int32, (SUBS, 128), 1)
    found = []
    for k in range(2):
        pick = jnp.where(source == peer[k] * EXTRA, 1.0, 0.0).astype(BF)
        line = contract(pick, routers, 1, 0)
        value = jnp.sum(jnp.where(lane == slot[k], line, 0.0), axis=1, keepdims=True)
        found.append(value / weight[k])
    both = jnp.where(lane == 0, found[0], jnp.where(lane == 1, found[1], 0.0))
    probs[...] = jnp.transpose(both)[0:8, :]


def combine_first(table, back):
    return pl.pallas_call(
        combine_first_kernel,
        out_shape=jax.ShapeDtypeStruct((SUBS, DS), F32),
        compiler_params=params(),
        name="combine_first",
    )(table, back)


def combine_last(table, part, back):
    return pl.pallas_call(
        combine_last_kernel,
        out_shape=[
            jax.ShapeDtypeStruct((SUBS // H, H * DS), BF),
            jax.ShapeDtypeStruct((8, SUBS), F32),
        ],
        compiler_params=params(),
        name="combine_last",
    )(table, part, back)


def final_kernel(which, own0, own1, own2, other, grad_in, grad_out):
    a = which[0]
    b = 1 - a
    for k in range(3):
        total = own0[k].astype(F32) + own1[k].astype(F32) + own2[k].astype(F32)
        total = total.astype(BF)
        if k < 2:
            grad_in[a, k] = total
            grad_in[b, k] = other[k]
        else:
            grad_out[a] = total
            grad_out[b] = other[k]


def final(which, own, other):
    vmem = pl.BlockSpec(memory_space=pltpu.VMEM)
    return pl.pallas_call(
        final_kernel,
        in_specs=[pl.BlockSpec(memory_space=pltpu.SMEM)] + [vmem] * 4,
        out_shape=[
            jax.ShapeDtypeStruct((2, 2, SH, DS), BF),
            jax.ShapeDtypeStruct((2, SH, DS), BF),
        ],
        compiler_params=params(),
        name="final",
    )(which, *own, other)


def ring(a, step):
    return lax.ppermute(a, "x", [(i, (i + step) % 4) for i in range(4)])


def swap(a):
    return lax.ppermute(a, "yh", [(0, 1), (1, 0)])


def exchange(a):
    return lax.all_to_all(a, PLANE, 0, 0, tiled=True)


def add(*arrays):
    return sum(a.astype(F32) for a in arrays).astype(BF)


def layer(tokens, cotangent, expert_ids, slot_ids, route_probs, weights_in, weights_out):
    yh = lax.axis_index("yh")
    both = jnp.concatenate([weights_in, weights_out[:, None]], axis=1)
    theirs = jnp.where(yh == 0, both[1], both[0])
    w_o = jnp.where(yh == 0, both[0], both[1])
    w_p = swap(theirs)
    w_o_m = ring(w_o, 1)
    w_o_p = ring(w_o, -1)
    w_p_m = ring(w_p, 1)
    w_p_p = ring(w_p, -1)
    w_o_2 = ring(w_o_p, -1)
    w_p_2 = ring(w_p_m, 1)

    dest = expert_ids % 2 * (PEERS // 2) + expert_ids // 2
    code = jnp.where(
        slot_ids < SLOTS[0],
        dest * SLOTS[0] + slot_ids,
        PEERS * SLOTS[0] + dest * SLOTS[1] + slot_ids - SLOTS[0],
    )
    table = [code, route_probs, dest, slot_ids]
    table = jnp.concatenate([t.astype(F32) for t in table], axis=2)
    table = jnp.transpose(table, (2, 1, 0)).reshape(8, SUBS)

    z1 = exchange(dispatch(table, tokens, cotangent, 0))
    z2 = exchange(dispatch(table, tokens, cotangent, 1))

    w_p = [w_p_2, w_p_p, w_p_m, w_p]
    w_o = [w_o_2, w_o_p, w_o_m, w_o]
    dw_p, *carry = expert_part(0, z1, w_p)
    dw_o, back1, router1 = expert_part(0, z1, w_o, carry=carry)
    back1 = exchange(back1)
    p_2, p_p, p_m, p_0, *carry = expert_part(1, z2, w_p, dw_p)
    p_2 = ring(p_2, 1)
    p_m = ring(p_m, -1)
    o_2, o_p, o_m, o_0, back2 = expert_part(1, z2, w_o, dw_o, carry, router1)
    back2 = exchange(back2)
    o_2 = ring(o_2, -1)
    p_p = ring(add(p_p, p_2), 1)
    o_p = ring(o_p, 1)
    o_m = ring(add(o_m, o_2), -1)
    other = swap(add(p_0, p_p, p_m))
    grad_in, grad_out = final(yh.astype(jnp.int32).reshape(1), (o_0, o_p, o_m), other)

    part = combine_first(table, back1)
    grad_tokens, probs = combine_last(table, part, back2)
    grad_probs = jnp.transpose(probs[0:2].reshape(2, H, SUBS // H), (2, 1, 0))
    return grad_tokens, grad_probs, grad_in, grad_out


def solution(mesh):
    wide = Mesh(mesh.devices.reshape(4, 2, 4, 2, 2), AXES)
    dp = ("x", "yh")
    expert = ("z", "yl", "core")
    rows2 = P(AXES, None)
    rows3 = P(AXES, None, None)
    w_in = P(expert, None, dp, None)
    w_out = P(expert, dp, None)
    return jax.shard_map(
        layer,
        mesh=wide,
        in_specs=(rows2, rows2, rows3, rows3, rows3, w_in, w_out),
        out_specs=(rows2, rows3, w_in, w_out),
        check_vma=False,
    )
```

```python
import functools

import jax
import jax.numpy as jnp
from jax import lax
from jax.experimental import pallas as pl
from jax.experimental.pallas import tpu as pltpu
from jax.sharding import Mesh
from jax.sharding import PartitionSpec as P

H = 8
DS = 512
PEERS = 32
SLOTS = (32, 32)
GROUP = 8
SUBS = 1024
EXTRA = 8
SH = 224
F32 = jnp.float32
BF = jnp.bfloat16
AXES = ("x", "yh", "z", "yl", "core")
PLANE = ("yh", "z", "yl", "core")


def contract(a, b, ca, cb):
    return lax.dot_general(a, b, (((ca,), (cb,)), ((), ())), preferred_element_type=F32)


def in_hbm(a):
    return pltpu.with_memory_space_constraint(a, pltpu.HBM)


def params(mib=24):
    return pltpu.CompilerParams(vmem_limit_bytes=mib * 2**20)


def dispatch_kernel(table, tok, cot, out, *, part):
    slots = SLOTS[part]
    base = part * PEERS * SLOTS[0]
    x = jnp.concatenate([tok[:, h * DS : (h + 1) * DS] for h in range(H)], axis=0)
    c = jnp.concatenate([cot[:, h * DS : (h + 1) * DS] for h in range(H)], axis=0)
    code0 = table[0:1, :].astype(jnp.int32)
    code1 = table[1:2, :].astype(jnp.int32)
    prob0 = table[2:3, :]
    prob1 = table[3:4, :]
    block = GROUP * slots
    row = lax.broadcasted_iota(jnp.int32, (block, SUBS), 0) + (base + pl.program_id(0) * block)
    hit0 = row == code0
    hit1 = row == code1
    scale = jnp.where(hit0, prob0, jnp.where(hit1, prob1, 0.0)).astype(BF)
    pick = jnp.where(hit0 | hit1, 1.0, 0.0).astype(BF)
    out[:, 0:slots, :] = contract(pick, x, 1, 0).astype(BF).reshape(GROUP, slots, DS)
    out[:, slots : 2 * slots, :] = contract(scale, c, 1, 0).astype(BF).reshape(GROUP, slots, DS)


def dispatch(table, tok, cot, part):
    slots = SLOTS[part]
    fixed = lambda b: (0, 0)
    return pl.pallas_call(
        functools.partial(dispatch_kernel, part=part),
        grid=(PEERS // GROUP,),
        in_specs=[
            pl.BlockSpec((8, SUBS), fixed),
            pl.BlockSpec((SUBS // H, H * DS), fixed),
            pl.BlockSpec((SUBS // H, H * DS), fixed),
        ],
        out_specs=pl.BlockSpec((GROUP, 2 * slots, DS), lambda b: (b, 0, 0)),
        out_shape=pltpu.HBM((PEERS, 2 * slots, DS), BF),
        compiler_params=params(),
    )(table, tok, cot)


HBM = pl.BlockSpec(memory_space=pltpu.HBM)
WHOLE = pl.BlockSpec(memory_space=pltpu.VMEM)
UNITS = 2 * SH
STEPS = 2


def expert_block(x, s, wg, wu, wo):
    hidden, rows = wg.shape[0], x.shape[0]
    g = contract(wg, x, 1, 1)
    u = contract(wu, x, 1, 1)
    dh = contract(wo, s, 1, 1)
    sig = 0.5 * jnp.tanh(0.5 * g) + 0.5
    act = g * sig
    hid = (act * u).astype(BF)
    dhu = dh * u
    du = (dh * act).astype(BF)
    dg = (dhu * (sig + act * (1.0 - sig))).astype(BF)
    router = jnp.sum((dhu * act).reshape(hidden // 8, 8, rows), axis=0)
    dw = (contract(dg, x, 1, 0), contract(du, x, 1, 0), contract(hid, s, 1, 0))
    dx = contract(dg, wg, 0, 0) + contract(du, wu, 0, 0)
    return dw, dx, router


def router_rows(back, slots, router_first, router):
    table = jnp.zeros((PEERS, 128), F32)
    for part, value in ((0, router_first), (1, router)):
        count = SLOTS[part]
        total = PEERS * count
        source = lax.broadcasted_iota(jnp.int32, (PEERS, total), 0) * count
        row = lax.broadcasted_iota(jnp.int32, (PEERS, total), 1)
        flat = jnp.sum(value, axis=0, keepdims=True)
        spread = jnp.where((row >= source) & (row < source + count), flat, 0.0).astype(BF)
        slot = lax.broadcasted_iota(jnp.int32, (total, 128), 0) % count + part * SLOTS[0]
        lane = lax.broadcasted_iota(jnp.int32, (total, 128), 1)
        place = jnp.where(slot == lane, 1.0, 0.0).astype(BF)
        table = table + contract(spread, place, 1, 0)
    back[:, slots : slots + EXTRA, 0:128] = jnp.broadcast_to(
        table.astype(BF)[:, None, :], (PEERS, EXTRA, 128)
    )
    back[:, slots : slots + EXTRA, 128:DS] = jnp.zeros((PEERS, EXTRA, DS - 128), BF)


def expert_kernel(*refs, part, pairs, first, begin, end):
    slots = SLOTS[part]
    step_peers = PEERS // STEPS
    step_rows = step_peers * slots
    last = part == 1 and end
    refs = list(refs)
    take = lambda n: [refs.pop(0) for _ in range(n)]
    (z_in,) = take(1)
    weights = take(2 * pairs)
    before = take(1)[0] if part else None
    acc_in, router_in = (None, None) if begin else take(2)
    router_first = take(1)[0] if last else None
    outs = take(2 * pairs if part else 1)
    (dx_out,) = take(1)
    router = None if last else take(1)[0]
    if last:
        router = refs.pop()
    z, acc, wbuf, stage, obuf, zsem, asem, wsem, bsem, ssem = refs

    def units(p):
        return pl.ds(pl.multiple_of(p * UNITS, UNITS), UNITS)

    def fetch(k, slot):
        half = k % 2
        return pltpu.make_async_copy(
            weights[k], wbuf.at[slot, :, half * SH : (half + 1) * SH, :], wsem.at[slot, half]
        )

    def load(p):
        return pltpu.make_async_copy(before.at[:, units(first + p), :], stage.at[p], bsem.at[p])

    def store_wide(p):
        return pltpu.make_async_copy(stage.at[p], outs[0].at[:, units(p), :], bsem.at[p])

    def store(p, half):
        return pltpu.make_async_copy(
            obuf.at[p, :, half * SH : (half + 1) * SH, :], outs[2 * p + half], ssem.at[p, half]
        )

    z_load = pltpu.make_async_copy(z_in, z, zsem)
    z_load.start()
    for k in range(2 * pairs):
        fetch(k, k // 2).start()
    if part:
        for p in range(pairs):
            load(p).start()
    else:
        stage[...] = jnp.zeros_like(stage)
    if begin:
        acc[...] = jnp.zeros_like(acc)
        router[...] = jnp.zeros_like(router)
    else:
        acc_load = pltpu.make_async_copy(acc_in, acc, asem)
        acc_load.start()
        router[...] = router_in[...]
    z_load.wait()

    def block(i, carry):
        p = i // STEPS
        b = i % STEPS

        @pl.when(b == 0)
        def _():
            fetch(0, p).wait()
            fetch(1, p).wait()

        here = pl.ds(b * step_peers, step_peers)
        x = z[here, 0:slots, :].reshape(step_rows, DS)
        s = z[here, slots : 2 * slots, :].reshape(step_rows, DS)
        parts, dx, r = expert_block(x, s, wbuf[p, 0], wbuf[p, 1], wbuf[p, 2])
        if part:

            @pl.when(b == 0)
            def _():
                load(p).wait()

        if not begin:

            @pl.when(i == 0)
            def _():
                acc_load.wait()

        for k in range(3):
            stage[p, k] += parts[k]
        acc[b] += dx
        router[b] += r

        @pl.when(b == STEPS - 1)
        def _():
            if part:
                obuf[p] = stage[p].astype(BF)
                for q in range(pairs):

                    @pl.when(p == q)
                    def _():
                        store(q, 0).start()
                        store(q, 1).start()
            else:
                store_wide(p).start()

        return carry

    lax.fori_loop(0, pairs * STEPS, block, 0)
    if end:
        dx_out[:, 0:slots, :] = acc[...].astype(BF).reshape(PEERS, slots, DS)
    else:
        acc_save = pltpu.make_async_copy(acc, dx_out, asem)
        acc_save.start()
    if last:
        flat = [jnp.concatenate([r[b] for b in range(STEPS)], axis=1) for r in (router_first, router)]
        router_rows(dx_out, slots, *flat)
    for p in range(pairs):
        if part:
            store(p, 0).wait()
            store(p, 1).wait()
        else:
            store_wide(p).wait()
    if not end:
        acc_save.wait()


def expert_part(part, z, weights, before=None, first=0, carry=None, end=False, router_first=None):
    pairs = len(weights) // 2
    slots = SLOTS[part]
    step_rows = PEERS // STEPS * slots
    last = part == 1 and end
    args = [z, *[in_hbm(w) for w in weights]]
    in_specs = [pl.BlockSpec(memory_space=pl.ANY)] + [HBM] * len(weights)
    if part:
        args += [in_hbm(before)]
        in_specs += [HBM]
    if carry is not None:
        args += [in_hbm(carry[0]), carry[1]]
        in_specs += [HBM, WHOLE]
    if last:
        args += [router_first]
        in_specs += [WHOLE]
    if part:
        out_shape = [pltpu.HBM((3, SH, DS), BF)] * (2 * pairs)
    else:
        out_shape = [pltpu.HBM((3, pairs * UNITS, DS), F32)]
    out_specs = [HBM] * len(out_shape)
    if end:
        out_shape += [pltpu.HBM((PEERS, slots + part * EXTRA, DS), BF)]
        out_specs += [WHOLE]
    else:
        out_shape += [pltpu.HBM((STEPS, step_rows, DS), F32)]
        out_specs += [HBM]
    if not last:
        out_shape += [jax.ShapeDtypeStruct((STEPS, 8, step_rows), F32)]
        out_specs += [WHOLE]
    return pl.pallas_call(
        functools.partial(
            expert_kernel, part=part, pairs=pairs, first=first, begin=carry is None, end=end
        ),
        in_specs=in_specs,
        out_specs=out_specs,
        out_shape=out_shape,
        scratch_shapes=[
            pltpu.VMEM((PEERS, 2 * slots, DS), BF),
            pltpu.VMEM((STEPS, step_rows, DS), F32),
            pltpu.VMEM((pairs, 3, UNITS, DS), BF),
            pltpu.VMEM((pairs, 3, UNITS, DS), F32),
            pltpu.VMEM((pairs, 3, UNITS, DS) if part else (8, 128), BF),
            pltpu.SemaphoreType.DMA,
            pltpu.SemaphoreType.DMA,
            pltpu.SemaphoreType.DMA((pairs, 2)),
            pltpu.SemaphoreType.DMA((pairs,)),
            pltpu.SemaphoreType.DMA((pairs, 2)),
            *([pltpu.VMEM((STEPS, 8, step_rows), F32)] if last else []),
        ],
        compiler_params=params(36),
    )(*args)


def picks(codes, part, start, count):
    rows = PEERS * SLOTS[part]
    row = lax.broadcasted_iota(jnp.int32, (count, rows), 1) + part * PEERS * SLOTS[0]
    code0, code1 = (c[start : start + count] for c in codes)
    return jnp.where((row == code0) | (row == code1), 1.0, 0.0).astype(BF)


def columns(table):
    cols = jnp.transpose(table[...])
    whole = lambda k: cols[:, k : k + 1].astype(jnp.int32)
    return (whole(0), whole(1)), (cols[:, 2:3], cols[:, 3:4]), (whole(4), whole(5)), (whole(6), whole(7))


def combine_first_kernel(table, back, out):
    codes = columns(table)[0]
    rows = back[...].reshape(PEERS * SLOTS[0], DS)
    count = 256
    for b in range(SUBS // count):
        out[b * count : (b + 1) * count, :] = contract(
            picks(codes, 0, b * count, count), rows, 1, 0
        )


def combine_last_kernel(table, part, back, out, probs):
    codes, weight, peer, slot = columns(table)
    rows = back[:, 0 : SLOTS[1], :].reshape(PEERS * SLOTS[1], DS)
    count = 256
    n = count // 128
    for b in range(SUBS // count):
        got = contract(picks(codes, 1, b * count, count), rows, 1, 0)
        got = (got + part[b * count : (b + 1) * count, :]).astype(BF)
        for k in range(n):
            h = b * n + k
            out[:, h * DS : (h + 1) * DS] = got[k * 128 : (k + 1) * 128]
    routers = back[:, SLOTS[1] : SLOTS[1] + EXTRA, 0:128].reshape(PEERS * EXTRA, 128)
    source = lax.broadcasted_iota(jnp.int32, (SUBS, PEERS * EXTRA), 1)
    lane = lax.broadcasted_iota(jnp.int32, (SUBS, 128), 1)
    found = []
    for k in range(2):
        pick = jnp.where(source == peer[k] * EXTRA, 1.0, 0.0).astype(BF)
        line = contract(pick, routers, 1, 0)
        value = jnp.sum(jnp.where(lane == slot[k], line, 0.0), axis=1, keepdims=True)
        found.append(value / weight[k])
    both = jnp.where(lane == 0, found[0], jnp.where(lane == 1, found[1], 0.0))
    probs[...] = jnp.transpose(both)[0:8, :]


def combine_first(table, back):
    return pl.pallas_call(
        combine_first_kernel,
        out_shape=jax.ShapeDtypeStruct((SUBS, DS), F32),
        compiler_params=params(),
        name="combine_first",
    )(table, back)


def combine_last(table, part, back):
    return pl.pallas_call(
        combine_last_kernel,
        out_shape=[
            jax.ShapeDtypeStruct((SUBS // H, H * DS), BF),
            jax.ShapeDtypeStruct((8, SUBS), F32),
        ],
        compiler_params=params(),
        name="combine_last",
    )(table, part, back)


def final_own_kernel(which, own0, own1, own2, grad_in, grad_out, total, sems):
    a = which[0]
    for k in range(3):
        value = own0[k].astype(F32) + own1[k].astype(F32) + own2[k].astype(F32)
        total[k] = value.astype(BF)
    copies = (
        pltpu.make_async_copy(total.at[0:2], grad_in.at[a], sems.at[0]),
        pltpu.make_async_copy(total.at[2], grad_out.at[a], sems.at[1]),
    )
    for c in copies:
        c.start()
    for c in copies:
        c.wait()


def final_other_kernel(which, other, _in, _out, grad_in, grad_out, sems):
    b = 1 - which[0]
    copies = (
        pltpu.make_async_copy(other.at[0:2], grad_in.at[b], sems.at[0]),
        pltpu.make_async_copy(other.at[2], grad_out.at[b], sems.at[1]),
    )
    for c in copies:
        c.start()
    for c in copies:
        c.wait()


def final(which, own, other):
    smem = pl.BlockSpec(memory_space=pltpu.SMEM)
    out_shape = [pltpu.HBM((2, 2, SH, DS), BF), pltpu.HBM((2, SH, DS), BF)]
    grads = pl.pallas_call(
        final_own_kernel,
        in_specs=[smem] + [WHOLE] * 3,
        out_specs=[HBM, HBM],
        out_shape=out_shape,
        scratch_shapes=[pltpu.VMEM((3, SH, DS), BF), pltpu.SemaphoreType.DMA((2,))],
        compiler_params=params(),
        name="final_own",
    )(which, *own)
    return pl.pallas_call(
        final_other_kernel,
        in_specs=[smem] + [HBM] * 3,
        out_specs=[HBM, HBM],
        out_shape=out_shape,
        input_output_aliases={2: 0, 3: 1},
        scratch_shapes=[pltpu.SemaphoreType.DMA((2,))],
        compiler_params=params(),
        name="final_other",
    )(which, in_hbm(other), *[in_hbm(g) for g in grads])


def ring(a, step):
    return lax.ppermute(a, "x", [(i, (i + step) % 4) for i in range(4)])


def swap(a):
    return lax.ppermute(a, "yh", [(0, 1), (1, 0)])


def exchange(a):
    return lax.all_to_all(a, PLANE, 0, 0, tiled=True)


def add(*arrays):
    return sum(a.astype(F32) for a in arrays).astype(BF)


def layer(tokens, cotangent, expert_ids, slot_ids, route_probs, weights_in, weights_out):
    yh = lax.axis_index("yh")
    both = jnp.concatenate([weights_in, weights_out[:, None]], axis=1)
    w_p = swap(jnp.where(yh == 0, both[1], both[0]))
    w_o = jnp.where(yh == 0, both[0], both[1])
    w_o_m = ring(w_o, 1)
    w_o_p = ring(w_o, -1)
    w_p_m = ring(w_p, 1)
    w_p_p = ring(w_p, -1)
    w_o_2 = ring(w_o_p, -1)
    w_p_2 = ring(w_p_m, 1)

    dest = expert_ids % 2 * (PEERS // 2) + expert_ids // 2
    code = jnp.where(
        slot_ids < SLOTS[0],
        dest * SLOTS[0] + slot_ids,
        PEERS * SLOTS[0] + dest * SLOTS[1] + slot_ids - SLOTS[0],
    )
    table = [code, route_probs, dest, slot_ids]
    table = jnp.concatenate([t.astype(F32) for t in table], axis=2)
    table = jnp.transpose(table, (2, 1, 0)).reshape(8, SUBS)

    z1 = exchange(dispatch(table, tokens, cotangent, 0))
    z2 = exchange(dispatch(table, tokens, cotangent, 1))

    near = [w_p_p, w_p_m, w_o_p, w_o_m]
    far = [w_p_2, w_o_2]
    own = [w_p, w_o]
    dw_near, *carry = expert_part(0, z1, near)
    dw_rest, back1, router1 = expert_part(0, z1, far + own, carry=carry, end=True)
    back1 = exchange(back1)
    p_2, o_2, *carry = expert_part(1, z2, far, dw_rest)
    p_2 = ring(p_2, 1)
    o_2 = ring(o_2, -1)
    p_p, p_m, o_p, o_m, *carry = expert_part(1, z2, near, dw_near, 0, carry)
    p_m = ring(p_m, -1)
    p_p = ring(add(p_p, p_2), 1)
    o_m = ring(add(o_m, o_2), -1)
    o_p = ring(o_p, 1)
    p_0, o_0, back2 = expert_part(1, z2, own, dw_rest, 1, carry, True, router1)
    back2 = exchange(back2)
    other = swap(add(p_0, p_p, p_m))
    grad_in, grad_out = final(yh.astype(jnp.int32).reshape(1), (o_0, o_p, o_m), other)

    part = combine_first(table, back1)
    grad_tokens, probs = combine_last(table, part, back2)
    grad_probs = jnp.transpose(probs[0:2].reshape(2, H, SUBS // H), (2, 1, 0))
    return grad_tokens, grad_probs, grad_in, grad_out


def solution(mesh):
    wide = Mesh(mesh.devices.reshape(4, 2, 4, 2, 2), AXES)
    dp = ("x", "yh")
    expert = ("z", "yl", "core")
    rows2 = P(AXES, None)
    rows3 = P(AXES, None, None)
    w_in = P(expert, None, dp, None)
    w_out = P(expert, dp, None)
    return jax.shard_map(
        layer,
        mesh=wide,
        in_specs=(rows2, rows2, rows3, rows3, rows3, w_in, w_out),
        out_specs=(rows2, rows3, w_in, w_out),
        check_vma=False,
    )
```

```python
import functools

import jax
import jax.numpy as jnp
from jax import lax
from jax.experimental import pallas as pl
from jax.experimental.pallas import tpu as pltpu
from jax.sharding import Mesh
from jax.sharding import PartitionSpec as P

H = 8
DS = 512
CAP = 64
PEERS = 32
SLOTS = (32, 32)
GROUP = 8
SUBS = 1024
EXTRA = 8
SH = 224
F32 = jnp.float32
BF = jnp.bfloat16
AXES = ("x", "yh", "z", "yl", "core")
PLANE = ("yh", "z", "yl", "core")


def contract(a, b, ca, cb):
    return lax.dot_general(a, b, (((ca,), (cb,)), ((), ())), preferred_element_type=F32)


def in_hbm(a):
    return pltpu.with_memory_space_constraint(a, pltpu.HBM)


def params(mib=24):
    return pltpu.CompilerParams(vmem_limit_bytes=mib * 2**20)


def dispatch_kernel(table, tok, cot, out, *, part):
    slots = SLOTS[part]
    base = part * PEERS * SLOTS[0]
    x = jnp.concatenate([tok[:, h * DS : (h + 1) * DS] for h in range(H)], axis=0)
    c = jnp.concatenate([cot[:, h * DS : (h + 1) * DS] for h in range(H)], axis=0)
    code0 = table[0:1, :].astype(jnp.int32)
    code1 = table[1:2, :].astype(jnp.int32)
    prob0 = table[2:3, :]
    prob1 = table[3:4, :]
    block = GROUP * slots
    row = lax.broadcasted_iota(jnp.int32, (block, SUBS), 0) + (base + pl.program_id(0) * block)
    hit0 = row == code0
    hit1 = row == code1
    scale = jnp.where(hit0, prob0, jnp.where(hit1, prob1, 0.0)).astype(BF)
    pick = jnp.where(hit0 | hit1, 1.0, 0.0).astype(BF)
    out[:, 0:slots, :] = contract(pick, x, 1, 0).astype(BF).reshape(GROUP, slots, DS)
    out[:, slots : 2 * slots, :] = contract(scale, c, 1, 0).astype(BF).reshape(GROUP, slots, DS)


def dispatch(table, tok, cot, part):
    slots = SLOTS[part]
    fixed = lambda b: (0, 0)
    return pl.pallas_call(
        functools.partial(dispatch_kernel, part=part),
        grid=(PEERS // GROUP,),
        in_specs=[
            pl.BlockSpec((8, SUBS), fixed),
            pl.BlockSpec((SUBS // H, H * DS), fixed),
            pl.BlockSpec((SUBS // H, H * DS), fixed),
        ],
        out_specs=pl.BlockSpec((GROUP, 2 * slots, DS), lambda b: (b, 0, 0)),
        out_shape=pltpu.HBM((PEERS, 2 * slots, DS), BF),
        compiler_params=params(),
    )(table, tok, cot)


def expert_block(z, slots, wg, wu, wo):
    hidden = wg.shape[0]
    rows = PEERS * slots
    x = z[:, 0:slots, :].reshape(rows, DS)
    s = z[:, slots : 2 * slots, :].reshape(rows, DS)
    g = contract(wg, x, 1, 1)
    u = contract(wu, x, 1, 1)
    dh = contract(wo, s, 1, 1)
    sig = 0.5 * jnp.tanh(0.5 * g) + 0.5
    act = g * sig
    hid = (act * u).astype(BF)
    dhu = dh * u
    du = (dh * act).astype(BF)
    dg = (dhu * (sig + act * (1.0 - sig))).astype(BF)
    router = jnp.sum((dhu * act).reshape(hidden // 8, 8, rows), axis=0)
    dw = (contract(dg, x, 1, 0), contract(du, x, 1, 0), contract(hid, s, 1, 0))
    dx = contract(dg, wg, 0, 0) + contract(du, wu, 0, 0)
    return dw, dx, router


HBM = pl.BlockSpec(memory_space=pltpu.HBM)
WHOLE = pl.BlockSpec(memory_space=pltpu.VMEM)
UNITS = 2 * SH


def router_rows(back, at, router_first, router):
    table = jnp.zeros((PEERS, 128), F32)
    for part, value in ((0, router_first), (1, router)):
        count = SLOTS[part]
        total = PEERS * count
        source = lax.broadcasted_iota(jnp.int32, (PEERS, total), 0) * count
        row = lax.broadcasted_iota(jnp.int32, (PEERS, total), 1)
        flat = jnp.sum(value, axis=0, keepdims=True)
        spread = jnp.where((row >= source) & (row < source + count), flat, 0.0).astype(BF)
        slot = lax.broadcasted_iota(jnp.int32, (total, 128), 0) % count + part * SLOTS[0]
        lane = lax.broadcasted_iota(jnp.int32, (total, 128), 1)
        place = jnp.where(slot == lane, 1.0, 0.0).astype(BF)
        table = table + contract(spread, place, 1, 0)
    back[:, at : at + EXTRA, 0:128] = jnp.broadcast_to(
        table.astype(BF)[:, None, :], (PEERS, EXTRA, 128)
    )
    back[:, at : at + EXTRA, 128:DS] = jnp.zeros((PEERS, EXTRA, DS - 128), BF)


def expert_kernel(*refs, part, end):
    slots = SLOTS[part]
    last = part == 1 and end
    refs = list(refs)
    take = lambda n: [refs.pop(0) for _ in range(n)]
    (z_in,) = take(1)
    weights = take(4)
    before = take(1)[0] if part else None
    acc_in, router_in = take(2) if end else (None, None)
    router_first = take(2)[0] if last else None
    outs = take(4 if part else 1)
    (dx_out,) = take(1)
    router_out = None if last else take(1)[0]
    z, acc, wbuf, stage, obuf, dbuf, zsem, asem, wsem, bsem, ssem = refs

    def units(p):
        return pl.ds(pl.multiple_of(p * UNITS, UNITS), UNITS)

    def fetch(k, slot):
        half = k % 2
        return pltpu.make_async_copy(
            weights[k], wbuf.at[slot, :, half * SH : (half + 1) * SH, :], wsem.at[slot, half]
        )

    def load(p):
        return pltpu.make_async_copy(before.at[:, units(p), :], stage.at[p], bsem.at[p])

    def store_wide(p):
        return pltpu.make_async_copy(stage.at[p], outs[0].at[:, units(p), :], bsem.at[p])

    def store(p, half):
        return pltpu.make_async_copy(
            obuf.at[p, :, half * SH : (half + 1) * SH, :], outs[2 * p + half], ssem.at[p, half]
        )

    z_load = pltpu.make_async_copy(z_in, z, zsem)
    z_load.start()
    for k in range(4):
        fetch(k, k // 2).start()
    if part:
        for p in range(2):
            load(p).start()
    if end:
        acc_load = pltpu.make_async_copy(acc_in, acc, asem)
        acc_load.start()
    else:
        acc[...] = jnp.zeros_like(acc)
    router = jnp.zeros((8, PEERS * slots), F32) if not end else router_in[...]
    z_load.wait()

    def block(p, router):
        fetch(0, p).wait()
        fetch(1, p).wait()
        parts, dx, r = expert_block(z, slots, wbuf[p, 0], wbuf[p, 1], wbuf[p, 2])
        if part:
            load(p).wait()
            for k in range(3):
                obuf[p, k] = (parts[k] + stage[p, k]).astype(BF)
            for q in range(2):

                @pl.when(p == q)
                def _():
                    for half in range(2):
                        store(q, half).start()
        else:
            for k in range(3):
                stage[p, k] = parts[k]
            store_wide(p).start()
        if end:

            @pl.when(p == 0)
            def _():
                acc_load.wait()

        acc[...] += dx
        return router + r

    router = lax.fori_loop(0, 2, block, router)
    if end:
        dbuf[:, 0:slots, :] = acc[...].astype(BF).reshape(PEERS, slots, DS)
        if last:
            router_rows(dbuf, slots, router_first[...], router)
        here = pl.ds(part * SLOTS[0], slots + part * EXTRA)
        save = pltpu.make_async_copy(dbuf, dx_out.at[:, here, :], asem)
    else:
        save = pltpu.make_async_copy(acc, dx_out, asem)
    save.start()
    if not last:
        router_out[...] = router
    for p in range(2):
        if part:
            store(p, 0).wait()
            store(p, 1).wait()
        else:
            store_wide(p).wait()
    save.wait()


def expert_part(part, z, weights, before=None, carry=None, first=None):
    end = carry is not None
    last = part == 1 and end
    slots = SLOTS[part]
    rows = PEERS * slots
    args = [z if part else in_hbm(z), *[in_hbm(w) for w in weights]]
    in_specs = [pl.BlockSpec(memory_space=pl.ANY) if part else HBM] + [HBM] * 4
    if part:
        args += [in_hbm(before)]
        in_specs += [HBM]
    if end:
        args += [in_hbm(carry[0]), carry[1]]
        in_specs += [HBM, WHOLE]
    if last:
        args += [first[1], in_hbm(first[0])]
        in_specs += [WHOLE, HBM]
    if part:
        out_shape = [pltpu.HBM((3, SH, DS), BF)] * 4
    else:
        out_shape = [pltpu.HBM((3, 4 * SH, DS), F32)]
    if end:
        out_shape += [pltpu.HBM((PEERS, CAP + EXTRA, DS), BF)]
    else:
        out_shape += [pltpu.HBM((rows, DS), F32)]
    out_specs = [HBM] * len(out_shape)
    if not last:
        out_shape += [jax.ShapeDtypeStruct((8, rows), F32)]
        out_specs += [WHOLE]
    return pl.pallas_call(
        functools.partial(expert_kernel, part=part, end=end),
        in_specs=in_specs,
        out_specs=out_specs,
        out_shape=out_shape,
        input_output_aliases={len(args) - 1: 4} if last else {},
        scratch_shapes=[
            pltpu.VMEM((PEERS, 2 * slots, DS), BF),
            pltpu.VMEM((rows, DS), F32),
            pltpu.VMEM((2, 3, UNITS, DS), BF),
            pltpu.VMEM((2, 3, UNITS, DS), F32),
            pltpu.VMEM((2, 3, UNITS, DS) if part else (8, 128), BF),
            pltpu.VMEM((PEERS, slots + part * EXTRA, DS) if end else (8, 128), BF),
            pltpu.SemaphoreType.DMA,
            pltpu.SemaphoreType.DMA,
            pltpu.SemaphoreType.DMA((2, 2)),
            pltpu.SemaphoreType.DMA((2,)),
            pltpu.SemaphoreType.DMA((2, 2)),
        ],
        compiler_params=params(36),
    )(*args)


def picks(codes, part, start, count):
    rows = PEERS * SLOTS[part]
    row = lax.broadcasted_iota(jnp.int32, (count, rows), 1) + part * PEERS * SLOTS[0]
    code0, code1 = (c[start : start + count] for c in codes)
    return jnp.where((row == code0) | (row == code1), 1.0, 0.0).astype(BF)


def columns(table):
    cols = jnp.transpose(table[...])
    whole = lambda k: cols[:, k : k + 1].astype(jnp.int32)
    return (whole(0), whole(1)), (cols[:, 2:3], cols[:, 3:4]), (whole(4), whole(5)), (whole(6), whole(7))


def combine_kernel(table, back, out, probs):
    codes, weight, peer, slot = columns(table)
    rows = [
        back[:, 0 : SLOTS[0], :].reshape(PEERS * SLOTS[0], DS),
        back[:, SLOTS[0] : CAP, :].reshape(PEERS * SLOTS[1], DS),
    ]
    count = 256
    n = count // 128
    for b in range(SUBS // count):
        got = contract(picks(codes, 0, b * count, count), rows[0], 1, 0)
        got = (got + contract(picks(codes, 1, b * count, count), rows[1], 1, 0)).astype(BF)
        for k in range(n):
            h = b * n + k
            out[:, h * DS : (h + 1) * DS] = got[k * 128 : (k + 1) * 128]
    routers = back[:, CAP : CAP + EXTRA, 0:128].reshape(PEERS * EXTRA, 128)
    source = lax.broadcasted_iota(jnp.int32, (SUBS, PEERS * EXTRA), 1)
    lane = lax.broadcasted_iota(jnp.int32, (SUBS, 128), 1)
    found = []
    for k in range(2):
        pick = jnp.where(source == peer[k] * EXTRA, 1.0, 0.0).astype(BF)
        line = contract(pick, routers, 1, 0)
        value = jnp.sum(jnp.where(lane == slot[k], line, 0.0), axis=1, keepdims=True)
        found.append(value / weight[k])
    both = jnp.where(lane == 0, found[0], jnp.where(lane == 1, found[1], 0.0))
    probs[...] = jnp.transpose(both)[0:8, :]


def combine(table, back):
    return pl.pallas_call(
        combine_kernel,
        out_shape=[
            jax.ShapeDtypeStruct((SUBS // H, H * DS), BF),
            jax.ShapeDtypeStruct((8, SUBS), F32),
        ],
        compiler_params=params(),
        name="combine",
    )(table, back)


def place(source, grad_in, grad_out, at, sems):
    copies = (
        pltpu.make_async_copy(source.at[0:2], grad_in.at[at], sems.at[0]),
        pltpu.make_async_copy(source.at[2], grad_out.at[at], sems.at[1]),
    )
    for c in copies:
        c.start()
    for c in copies:
        c.wait()


def final_own_kernel(which, own0, own1, own2, grad_in, grad_out, total, sems):
    for k in range(3):
        value = own0[k].astype(F32) + own1[k].astype(F32) + own2[k].astype(F32)
        total[k] = value.astype(BF)
    place(total, grad_in, grad_out, which[0], sems)


def final_other_kernel(which, other, _in, _out, grad_in, grad_out, sems):
    place(other, grad_in, grad_out, 1 - which[0], sems)


def final(which, own, other):
    smem = pl.BlockSpec(memory_space=pltpu.SMEM)
    out_shape = [pltpu.HBM((2, 2, SH, DS), BF), pltpu.HBM((2, SH, DS), BF)]
    grads = pl.pallas_call(
        final_own_kernel,
        in_specs=[smem] + [WHOLE] * 3,
        out_specs=[HBM, HBM],
        out_shape=out_shape,
        scratch_shapes=[pltpu.VMEM((3, SH, DS), BF), pltpu.SemaphoreType.DMA((2,))],
        compiler_params=params(),
        name="final_own",
    )(which, *own)
    return pl.pallas_call(
        final_other_kernel,
        in_specs=[smem, WHOLE, HBM, HBM],
        out_specs=[HBM, HBM],
        out_shape=out_shape,
        input_output_aliases={2: 0, 3: 1},
        scratch_shapes=[pltpu.SemaphoreType.DMA((2,))],
        compiler_params=params(),
        name="final_other",
    )(which, other, *[in_hbm(g) for g in grads])


def ring(a, step):
    return lax.ppermute(a, "x", [(i, (i + step) % 4) for i in range(4)])


def swap(a):
    return lax.ppermute(a, "yh", [(0, 1), (1, 0)])


def exchange(a):
    return lax.all_to_all(a, PLANE, 0, 0, tiled=True)


def add(*arrays):
    return sum(a.astype(F32) for a in arrays).astype(BF)


def layer(tokens, cotangent, expert_ids, slot_ids, route_probs, weights_in, weights_out):
    yh = lax.axis_index("yh")
    both = jnp.concatenate([weights_in, weights_out[:, None]], axis=1)
    w_p = swap(jnp.where(yh == 0, both[1], both[0]))
    w_o = jnp.where(yh == 0, both[0], both[1])
    w_o_m = ring(w_o, 1)
    w_o_p = ring(w_o, -1)
    w_p_m = ring(w_p, 1)
    w_p_p = ring(w_p, -1)
    w_o_2 = ring(w_o_p, -1)
    w_p_2 = ring(w_p_m, 1)

    dest = expert_ids % 2 * (PEERS // 2) + expert_ids // 2
    code = jnp.where(
        slot_ids < SLOTS[0],
        dest * SLOTS[0] + slot_ids,
        PEERS * SLOTS[0] + dest * SLOTS[1] + slot_ids - SLOTS[0],
    )
    table = [code, route_probs, dest, slot_ids]
    table = jnp.concatenate([t.astype(F32) for t in table], axis=2)
    table = jnp.transpose(table, (2, 1, 0)).reshape(8, SUBS)

    z1 = exchange(dispatch(table, tokens, cotangent, 0))
    z2 = exchange(dispatch(table, tokens, cotangent, 1))

    far = [w_p_2, w_o_2, w_p_p, w_p_m]
    rest = [w_o_p, w_o_m, w_p, w_o]
    dw_rest, *carry = expert_part(0, z1, rest)
    dw_far, *first = expert_part(0, z1, far, carry=carry)
    p_2, o_2, p_p, p_m, *carry = expert_part(1, z2, far, dw_far)
    p_2 = ring(p_2, 1)
    o_2 = ring(o_2, -1)
    p_m = ring(p_m, -1)
    o_p, o_m, p_0, o_0, back = expert_part(1, z2, rest, dw_rest, carry, first)
    back = exchange(back)
    p_p = ring(add(p_p, p_2), 1)
    o_m = ring(add(o_m, o_2), -1)
    o_p = ring(o_p, 1)
    other = swap(add(p_0, p_p, p_m))
    grad_in, grad_out = final(yh.astype(jnp.int32).reshape(1), (o_0, o_p, o_m), other)

    grad_tokens, probs = combine(table, back)
    grad_probs = jnp.transpose(probs[0:2].reshape(2, H, SUBS // H), (2, 1, 0))
    return grad_tokens, grad_probs, grad_in, grad_out


def solution(mesh):
    wide = Mesh(mesh.devices.reshape(4, 2, 4, 2, 2), AXES)
    dp = ("x", "yh")
    expert = ("z", "yl", "core")
    rows2 = P(AXES, None)
    rows3 = P(AXES, None, None)
    w_in = P(expert, None, dp, None)
    w_out = P(expert, dp, None)
    return jax.shard_map(
        layer,
        mesh=wide,
        in_specs=(rows2, rows2, rows3, rows3, rows3, w_in, w_out),
        out_specs=(rows2, rows3, w_in, w_out),
        check_vma=False,
    )
```

```python
import functools

import jax
import jax.numpy as jnp
from jax import lax
from jax.experimental import pallas as pl
from jax.experimental.pallas import tpu as pltpu
from jax.sharding import Mesh
from jax.sharding import PartitionSpec as P

H = 8
DS = 512
PEERS = 32
SLOTS = (40, 24)
GROUP = 8
SUBS = 1024
EXTRA = 8
SH = 224
F32 = jnp.float32
BF = jnp.bfloat16
AXES = ("x", "yh", "z", "yl", "core")
PLANE = ("yh", "z", "yl", "core")


def contract(a, b, ca, cb):
    return lax.dot_general(a, b, (((ca,), (cb,)), ((), ())), preferred_element_type=F32)


def in_hbm(a):
    return pltpu.with_memory_space_constraint(a, pltpu.HBM)


def params(mib=24):
    return pltpu.CompilerParams(vmem_limit_bytes=mib * 2**20)


def dispatch_kernel(table, tok, cot, out, *, part):
    slots = SLOTS[part]
    base = part * PEERS * SLOTS[0]
    x = jnp.concatenate([tok[:, h * DS : (h + 1) * DS] for h in range(H)], axis=0)
    c = jnp.concatenate([cot[:, h * DS : (h + 1) * DS] for h in range(H)], axis=0)
    code0 = table[0:1, :].astype(jnp.int32)
    code1 = table[1:2, :].astype(jnp.int32)
    prob0 = table[2:3, :]
    prob1 = table[3:4, :]
    block = GROUP * slots
    row = lax.broadcasted_iota(jnp.int32, (block, SUBS), 0) + (base + pl.program_id(0) * block)
    hit0 = row == code0
    hit1 = row == code1
    scale = jnp.where(hit0, prob0, jnp.where(hit1, prob1, 0.0)).astype(BF)
    pick = jnp.where(hit0 | hit1, 1.0, 0.0).astype(BF)
    out[:, 0:slots, :] = contract(pick, x, 1, 0).astype(BF).reshape(GROUP, slots, DS)
    out[:, slots : 2 * slots, :] = contract(scale, c, 1, 0).astype(BF).reshape(GROUP, slots, DS)


def dispatch(table, tok, cot, part):
    slots = SLOTS[part]
    fixed = lambda b: (0, 0)
    return pl.pallas_call(
        functools.partial(dispatch_kernel, part=part),
        grid=(PEERS // GROUP,),
        in_specs=[
            pl.BlockSpec((8, SUBS), fixed),
            pl.BlockSpec((SUBS // H, H * DS), fixed),
            pl.BlockSpec((SUBS // H, H * DS), fixed),
        ],
        out_specs=pl.BlockSpec((GROUP, 2 * slots, DS), lambda b: (b, 0, 0)),
        out_shape=pltpu.HBM((PEERS, 2 * slots, DS), BF),
        compiler_params=params(),
    )(table, tok, cot)


def expert_block(z, slots, wg, wu, wo):
    hidden = wg.shape[0]
    rows = PEERS * slots
    x = z[:, 0:slots, :].reshape(rows, DS)
    s = z[:, slots : 2 * slots, :].reshape(rows, DS)
    g = contract(wg, x, 1, 1)
    u = contract(wu, x, 1, 1)
    dh = contract(wo, s, 1, 1)
    sig = 0.5 * jnp.tanh(0.5 * g) + 0.5
    act = g * sig
    hid = (act * u).astype(BF)
    dhu = dh * u
    du = (dh * act).astype(BF)
    dg = (dhu * (sig + act * (1.0 - sig))).astype(BF)
    router = jnp.sum((dhu * act).reshape(hidden // 8, 8, rows), axis=0)
    dw = (contract(dg, x, 1, 0), contract(du, x, 1, 0), contract(hid, s, 1, 0))
    dx = contract(dg, wg, 0, 0) + contract(du, wu, 0, 0)
    return dw, dx, router


HBM = pl.BlockSpec(memory_space=pltpu.HBM)
WHOLE = pl.BlockSpec(memory_space=pltpu.VMEM)
UNITS = 2 * SH


def router_rows(back, at, router_first, router):
    table = jnp.zeros((PEERS, 128), F32)
    for part, value in ((0, router_first), (1, router)):
        count = SLOTS[part]
        total = PEERS * count
        source = lax.broadcasted_iota(jnp.int32, (PEERS, total), 0) * count
        row = lax.broadcasted_iota(jnp.int32, (PEERS, total), 1)
        flat = jnp.sum(value, axis=0, keepdims=True)
        spread = jnp.where((row >= source) & (row < source + count), flat, 0.0).astype(BF)
        slot = lax.broadcasted_iota(jnp.int32, (total, 128), 0) % count + part * SLOTS[0]
        lane = lax.broadcasted_iota(jnp.int32, (total, 128), 1)
        place = jnp.where(slot == lane, 1.0, 0.0).astype(BF)
        table = table + contract(spread, place, 1, 0)
    back[:, :, at : at + 128] = jnp.broadcast_to(table.astype(BF)[:, None, :], (PEERS, EXTRA, 128))


def expert_kernel(*refs, part, pairs, first, begin, end):
    slots = SLOTS[part]
    last = part == 1 and end
    refs = list(refs)
    take = lambda n: [refs.pop(0) for _ in range(n)]
    (z_in,) = take(1)
    weights = take(2 * pairs)
    before = take(1)[0] if part else None
    acc_in, router_in = (None, None) if begin else take(2)
    router_first = take(1)[0] if last else None
    outs = take(2 * pairs if part else 1)
    (dx_out,) = take(1)
    router_out = None if last else take(1)[0]
    z, acc, wbuf, stage, obuf, dbuf, zsem, asem, wsem, bsem, ssem = refs

    def units(p):
        return pl.ds(pl.multiple_of(p * UNITS, UNITS), UNITS)

    def fetch(k, slot):
        half = k % 2
        return pltpu.make_async_copy(
            weights[k], wbuf.at[slot, :, half * SH : (half + 1) * SH, :], wsem.at[slot, half]
        )

    def load(p):
        return pltpu.make_async_copy(before.at[:, units(first + p), :], stage.at[p], bsem.at[p])

    def store_wide(p):
        return pltpu.make_async_copy(stage.at[p], outs[0].at[:, units(p), :], bsem.at[p])

    def store(p, half):
        return pltpu.make_async_copy(
            obuf.at[p, :, half * SH : (half + 1) * SH, :], outs[2 * p + half], ssem.at[p, half]
        )

    if part:
        z = z_in
    else:
        z_load = pltpu.make_async_copy(z_in, z, zsem)
        z_load.start()
    for k in range(2 * pairs):
        fetch(k, k // 2).start()
    if part:
        for p in range(pairs):
            load(p).start()
    if not begin:
        acc_load = pltpu.make_async_copy(acc_in, acc, asem)
        acc_load.start()
    else:
        acc[...] = jnp.zeros_like(acc)
    router = jnp.zeros((8, PEERS * slots), F32) if begin else router_in[...]
    if not part:
        z_load.wait()

    def block(p, router):
        fetch(0, p).wait()
        fetch(1, p).wait()
        parts, dx, r = expert_block(z, slots, wbuf[p, 0], wbuf[p, 1], wbuf[p, 2])
        if part:
            load(p).wait()
            for k in range(3):
                obuf[p, k] = (parts[k] + stage[p, k]).astype(BF)
            for q in range(pairs):

                @pl.when(p == q)
                def _():
                    for half in range(2):
                        store(q, half).start()
        else:
            for k in range(3):
                stage[p, k] = parts[k]
            store_wide(p).start()
        if not begin:

            @pl.when(p == 0)
            def _():
                acc_load.wait()

        acc[...] += dx
        return router + r

    router = block(0, router) if pairs == 1 else lax.fori_loop(0, pairs, block, router)
    if end:
        rows = acc[...].astype(BF).reshape(PEERS, slots, DS)
        for g in range(slots // EXTRA):
            dbuf[:, :, g * DS : (g + 1) * DS] = rows[:, g * EXTRA : (g + 1) * EXTRA, :]
        if last:
            router_rows(dbuf, slots // EXTRA * DS, router_first[...], router)
        save = pltpu.make_async_copy(dbuf, dx_out, asem)
    else:
        save = pltpu.make_async_copy(acc, dx_out, asem)
    save.start()
    if not last:
        router_out[...] = router
    for p in range(pairs):
        if part:
            store(p, 0).wait()
            store(p, 1).wait()
        else:
            store_wide(p).wait()
    save.wait()


def expert_part(part, z, weights, before=None, at=0, carry=None, end=False, first=None):
    pairs = len(weights) // 2
    last = part == 1 and end
    slots = SLOTS[part]
    rows = PEERS * slots
    width = slots // EXTRA * DS + (128 if last else 0)
    args = [z if part else in_hbm(z), *[in_hbm(w) for w in weights]]
    in_specs = [WHOLE if part else HBM] + [HBM] * len(weights)
    if part:
        args += [in_hbm(before)]
        in_specs += [HBM]
    if carry is not None:
        args += [in_hbm(carry[0]), carry[1]]
        in_specs += [HBM, WHOLE]
    if last:
        args += [first]
        in_specs += [WHOLE]
    if part:
        out_shape = [pltpu.HBM((3, SH, DS), BF)] * (2 * pairs)
    else:
        out_shape = [pltpu.HBM((3, pairs * UNITS, DS), F32)]
    if end:
        out_shape += [pltpu.HBM((PEERS, EXTRA, width), BF)]
    else:
        out_shape += [pltpu.HBM((rows, DS), F32)]
    out_specs = [HBM] * len(out_shape)
    if not last:
        out_shape += [jax.ShapeDtypeStruct((8, rows), F32)]
        out_specs += [WHOLE]
    return pl.pallas_call(
        functools.partial(
            expert_kernel, part=part, pairs=pairs, first=at, begin=carry is None, end=end
        ),
        in_specs=in_specs,
        out_specs=out_specs,
        out_shape=out_shape,
        scratch_shapes=[
            pltpu.VMEM((8, 128, 128) if part else (PEERS, 2 * slots, DS), BF),
            pltpu.VMEM((rows, DS), F32),
            pltpu.VMEM((pairs, 3, UNITS, DS), BF),
            pltpu.VMEM((pairs, 3, UNITS, DS), F32),
            pltpu.VMEM((pairs, 3, UNITS, DS) if part else (8, 128), BF),
            pltpu.VMEM((PEERS, EXTRA, width) if end else (8, 128), BF),
            pltpu.SemaphoreType.DMA,
            pltpu.SemaphoreType.DMA,
            pltpu.SemaphoreType.DMA((pairs, 2)),
            pltpu.SemaphoreType.DMA((pairs,)),
            pltpu.SemaphoreType.DMA((pairs, 2)),
        ],
        compiler_params=params(44),
    )(*args)


def picks(codes, part, start, count):
    rows = PEERS * SLOTS[part]
    row = lax.broadcasted_iota(jnp.int32, (count, rows), 1) + part * PEERS * SLOTS[0]
    code0, code1 = (c[start : start + count] for c in codes)
    return jnp.where((row == code0) | (row == code1), 1.0, 0.0).astype(BF)


def columns(table):
    cols = jnp.transpose(table[...])
    whole = lambda k: cols[:, k : k + 1].astype(jnp.int32)
    return (whole(0), whole(1)), (cols[:, 2:3], cols[:, 3:4]), (whole(4), whole(5)), (whole(6), whole(7))


def slot_rows(back, part):
    slots = SLOTS[part]
    groups = [back[:, :, g * DS : (g + 1) * DS] for g in range(slots // EXTRA)]
    return jnp.concatenate(groups, axis=1).reshape(PEERS * slots, DS)


def combine_first_kernel(table, back, out):
    codes = columns(table)[0]
    rows = slot_rows(back, 0)
    count = 256
    for b in range(SUBS // count):
        out[b * count : (b + 1) * count, :] = contract(
            picks(codes, 0, b * count, count), rows, 1, 0
        )


def combine_last_kernel(table, part, back, out, probs):
    codes, weight, peer, slot = columns(table)
    rows = slot_rows(back, 1)
    count = 256
    n = count // 128
    for b in range(SUBS // count):
        got = contract(picks(codes, 1, b * count, count), rows, 1, 0)
        got = (got + part[b * count : (b + 1) * count, :]).astype(BF)
        for k in range(n):
            h = b * n + k
            out[:, h * DS : (h + 1) * DS] = got[k * 128 : (k + 1) * 128]
    at = SLOTS[1] // EXTRA * DS
    routers = back[:, :, at : at + 128].reshape(PEERS * EXTRA, 128)
    source = lax.broadcasted_iota(jnp.int32, (SUBS, PEERS * EXTRA), 1)
    lane = lax.broadcasted_iota(jnp.int32, (SUBS, 128), 1)
    found = []
    for k in range(2):
        pick = jnp.where(source == peer[k] * EXTRA, 1.0, 0.0).astype(BF)
        line = contract(pick, routers, 1, 0)
        value = jnp.sum(jnp.where(lane == slot[k], line, 0.0), axis=1, keepdims=True)
        found.append(value / weight[k])
    both = jnp.where(lane == 0, found[0], jnp.where(lane == 1, found[1], 0.0))
    probs[...] = jnp.transpose(both)[0:8, :]


def combine_first(table, back):
    return pl.pallas_call(
        combine_first_kernel,
        out_shape=jax.ShapeDtypeStruct((SUBS, DS), F32),
        compiler_params=params(),
        name="combine_first",
    )(table, in_hbm(back))


def combine_last(table, part, back):
    return pl.pallas_call(
        combine_last_kernel,
        out_shape=[
            jax.ShapeDtypeStruct((SUBS // H, H * DS), BF),
            jax.ShapeDtypeStruct((8, SUBS), F32),
        ],
        compiler_params=params(),
        name="combine_last",
    )(table, part, back)


def place(sources, grad_in, grad_out, at, sems):
    copies = []
    start = 0
    for i, source in enumerate(sources):
        here = pl.ds(start, source.shape[1])
        start += source.shape[1]
        copies += [
            pltpu.make_async_copy(source.at[0:2], grad_in.at[at, :, here, :], sems.at[i, 0]),
            pltpu.make_async_copy(source.at[2], grad_out.at[at, here, :], sems.at[i, 1]),
        ]
    for c in copies:
        c.start()
    for c in copies:
        c.wait()


def final_own_kernel(which, own0, own1, own2, own3, grad_in, grad_out, total, sems):
    for k in range(3):
        value = own0[k].astype(F32) + own1[k].astype(F32) + own2[k].astype(F32)
        total[k] = (value + own3[k].astype(F32)).astype(BF)
    place([total], grad_in, grad_out, which[0], sems)


def final_other_kernel(which, other, _in, _out, grad_in, grad_out, sems):
    place([other], grad_in, grad_out, 1 - which[0], sems)


def final(which, own, other):
    smem = pl.BlockSpec(memory_space=pltpu.SMEM)
    out_shape = [pltpu.HBM((2, 2, SH, DS), BF), pltpu.HBM((2, SH, DS), BF)]
    grads = pl.pallas_call(
        final_own_kernel,
        in_specs=[smem] + [WHOLE] * 4,
        out_specs=[HBM, HBM],
        out_shape=out_shape,
        scratch_shapes=[pltpu.VMEM((3, SH, DS), BF), pltpu.SemaphoreType.DMA((1, 2))],
        compiler_params=params(),
        name="final_own",
    )(which, *own)
    return pl.pallas_call(
        final_other_kernel,
        in_specs=[smem, WHOLE, HBM, HBM],
        out_specs=[HBM, HBM],
        out_shape=out_shape,
        input_output_aliases={2: 0, 3: 1},
        scratch_shapes=[pltpu.SemaphoreType.DMA((1, 2))],
        compiler_params=params(),
        name="final_other",
    )(which, other, *[in_hbm(g) for g in grads])


def ring(a, step):
    return lax.ppermute(a, "x", [(i, (i + step) % 4) for i in range(4)])


def swap(a):
    return lax.ppermute(a, "yh", [(0, 1), (1, 0)])


def exchange(a):
    return lax.all_to_all(a, PLANE, 0, 0, tiled=True)


def add(*arrays):
    return sum(a.astype(F32) for a in arrays).astype(BF)


def layer(tokens, cotangent, expert_ids, slot_ids, route_probs, weights_in, weights_out):
    yh = lax.axis_index("yh")
    both = jnp.concatenate([weights_in, weights_out[:, None]], axis=1)
    w_p = swap(jnp.where(yh == 0, both[1], both[0]))
    w_o = jnp.where(yh == 0, both[0], both[1])
    w_o_m = ring(w_o, 1)
    w_o_p = ring(w_o, -1)
    w_p_m = ring(w_p, 1)
    w_p_p = ring(w_p, -1)
    w_o_2 = ring(w_o_p, -1)
    w_p_2 = ring(w_p_m, 1)

    dest = expert_ids % 2 * (PEERS // 2) + expert_ids // 2
    code = jnp.where(
        slot_ids < SLOTS[0],
        dest * SLOTS[0] + slot_ids,
        PEERS * SLOTS[0] + dest * SLOTS[1] + slot_ids - SLOTS[0],
    )
    table = [code, route_probs, dest, slot_ids]
    table = jnp.concatenate([t.astype(F32) for t in table], axis=2)
    table = jnp.transpose(table, (2, 1, 0)).reshape(8, SUBS)

    z1 = exchange(dispatch(table, tokens, cotangent, 0))
    z2 = exchange(dispatch(table, tokens, cotangent, 1))

    near = [w_p_p, w_p_m, w_o_p, w_o_m]
    far = [w_p_2, w_o_2]
    own = [w_p, w_o]
    dw_near, *carry = expert_part(0, z1, near)
    dw_rest, back1, router1 = expert_part(0, z1, far + own, carry=carry, end=True)
    back1 = exchange(back1)
    p_2, o_2, *carry = expert_part(1, z2, far, dw_rest, 0)
    p_2 = ring(p_2, 2)
    o_2 = ring(o_2, 2)
    p_p, p_m, o_p, o_m, *carry = expert_part(1, z2, near, dw_near, 0, carry)
    p_p = ring(p_p, 1)
    p_m = ring(p_m, -1)
    o_p = ring(o_p, 1)
    o_m = ring(o_m, -1)
    p_0, o_0, back2 = expert_part(1, z2, own, dw_rest, 1, carry, True, router1)
    back2 = exchange(back2)
    other = swap(add(p_0, p_p, p_m, p_2))
    grad_in, grad_out = final(yh.astype(jnp.int32).reshape(1), (o_0, o_p, o_m, o_2), other)

    part = combine_first(table, back1)
    grad_tokens, probs = combine_last(table, part, back2)
    grad_probs = jnp.transpose(probs[0:2].reshape(2, H, SUBS // H), (2, 1, 0))
    return grad_tokens, grad_probs, grad_in, grad_out


def solution(mesh):
    wide = Mesh(mesh.devices.reshape(4, 2, 4, 2, 2), AXES)
    dp = ("x", "yh")
    expert = ("z", "yl", "core")
    rows2 = P(AXES, None)
    rows3 = P(AXES, None, None)
    w_in = P(expert, None, dp, None)
    w_out = P(expert, dp, None)
    return jax.shard_map(
        layer,
        mesh=wide,
        in_specs=(rows2, rows2, rows3, rows3, rows3, w_in, w_out),
        out_specs=(rows2, rows3, w_in, w_out),
        check_vma=False,
    )
```

```python
import functools

import jax
import jax.numpy as jnp
from jax import lax
from jax.experimental import pallas as pl
from jax.experimental.pallas import tpu as pltpu
from jax.sharding import Mesh
from jax.sharding import PartitionSpec as P

H = 8
DS = 512
CAP = 64
PEERS = 32
SLOTS = (32, 32)
GROUP = 8
SUBS = 1024
EXTRA = 8
SH = 224
F32 = jnp.float32
BF = jnp.bfloat16
AXES = ("x", "yh", "z", "yl", "core")
PLANE = ("yh", "z", "yl", "core")


def contract(a, b, ca, cb):
    return lax.dot_general(a, b, (((ca,), (cb,)), ((), ())), preferred_element_type=F32)


def in_hbm(a):
    return pltpu.with_memory_space_constraint(a, pltpu.HBM)


def params(mib=24):
    return pltpu.CompilerParams(vmem_limit_bytes=mib * 2**20)


def dispatch_kernel(table, tok, cot, out, *, part):
    slots = SLOTS[part]
    base = part * PEERS * SLOTS[0]
    x = jnp.concatenate([tok[:, h * DS : (h + 1) * DS] for h in range(H)], axis=0)
    c = jnp.concatenate([cot[:, h * DS : (h + 1) * DS] for h in range(H)], axis=0)
    code0 = table[0:1, :].astype(jnp.int32)
    code1 = table[1:2, :].astype(jnp.int32)
    prob0 = table[2:3, :]
    prob1 = table[3:4, :]
    block = GROUP * slots
    row = lax.broadcasted_iota(jnp.int32, (block, SUBS), 0) + (base + pl.program_id(0) * block)
    hit0 = row == code0
    hit1 = row == code1
    scale = jnp.where(hit0, prob0, jnp.where(hit1, prob1, 0.0)).astype(BF)
    pick = jnp.where(hit0 | hit1, 1.0, 0.0).astype(BF)
    out[:, 0:slots, :] = contract(pick, x, 1, 0).astype(BF).reshape(GROUP, slots, DS)
    out[:, slots : 2 * slots, :] = contract(scale, c, 1, 0).astype(BF).reshape(GROUP, slots, DS)


def dispatch(table, tok, cot, part):
    slots = SLOTS[part]
    fixed = lambda b: (0, 0)
    return pl.pallas_call(
        functools.partial(dispatch_kernel, part=part),
        grid=(PEERS // GROUP,),
        in_specs=[
            pl.BlockSpec((8, SUBS), fixed),
            pl.BlockSpec((SUBS // H, H * DS), fixed),
            pl.BlockSpec((SUBS // H, H * DS), fixed),
        ],
        out_specs=pl.BlockSpec((GROUP, 2 * slots, DS), lambda b: (b, 0, 0)),
        out_shape=pltpu.HBM((PEERS, 2 * slots, DS), BF),
        compiler_params=params(),
    )(table, tok, cot)


def expert_block(z, slots, wg, wu, wo):
    hidden = wg.shape[0]
    rows = PEERS * slots
    x = z[:, 0:slots, :].reshape(rows, DS)
    s = z[:, slots : 2 * slots, :].reshape(rows, DS)
    g = contract(wg, x, 1, 1)
    u = contract(wu, x, 1, 1)
    dh = contract(wo, s, 1, 1)
    sig = 0.5 * jnp.tanh(0.5 * g) + 0.5
    act = g * sig
    hid = (act * u).astype(BF)
    dhu = dh * u
    du = (dh * act).astype(BF)
    dg = (dhu * (sig + act * (1.0 - sig))).astype(BF)
    router = jnp.sum((dhu * act).reshape(hidden // 8, 8, rows), axis=0)
    dw = (contract(dg, x, 1, 0), contract(du, x, 1, 0), contract(hid, s, 1, 0))
    dx = contract(dg, wg, 0, 0) + contract(du, wu, 0, 0)
    return dw, dx, router


HBM = pl.BlockSpec(memory_space=pltpu.HBM)
WHOLE = pl.BlockSpec(memory_space=pltpu.VMEM)
UNITS = 2 * SH


def router_rows(back, at, router_first, router):
    table = jnp.zeros((PEERS, 128), F32)
    for part, value in ((0, router_first), (1, router)):
        count = SLOTS[part]
        total = PEERS * count
        source = lax.broadcasted_iota(jnp.int32, (PEERS, total), 0) * count
        row = lax.broadcasted_iota(jnp.int32, (PEERS, total), 1)
        flat = jnp.sum(value, axis=0, keepdims=True)
        spread = jnp.where((row >= source) & (row < source + count), flat, 0.0).astype(BF)
        slot = lax.broadcasted_iota(jnp.int32, (total, 128), 0) % count + part * SLOTS[0]
        lane = lax.broadcasted_iota(jnp.int32, (total, 128), 1)
        place = jnp.where(slot == lane, 1.0, 0.0).astype(BF)
        table = table + contract(spread, place, 1, 0)
    back[:, :, at : at + 128] = jnp.broadcast_to(table.astype(BF)[:, None, :], (PEERS, EXTRA, 128))


def expert_kernel(*refs, part, pairs, first, begin, end):
    slots = SLOTS[part]
    last = part == 1 and end
    refs = list(refs)
    take = lambda n: [refs.pop(0) for _ in range(n)]
    (z_in,) = take(1)
    weights = take(2 * pairs)
    before = take(1)[0] if part else None
    acc_in, router_in = (None, None) if begin else take(2)
    router_first = take(2)[0] if last else None
    outs = take(2 * pairs if part else 1)
    (dx_out,) = take(1)
    router_out = None if last else take(1)[0]
    z, acc, wbuf, stage, obuf, dbuf, zsem, asem, wsem, bsem, ssem = refs

    def units(p):
        return pl.ds(pl.multiple_of(p * UNITS, UNITS), UNITS)

    def fetch(k, slot):
        half = k % 2
        return pltpu.make_async_copy(
            weights[k], wbuf.at[slot, :, half * SH : (half + 1) * SH, :], wsem.at[slot, half]
        )

    def load(p):
        return pltpu.make_async_copy(before.at[:, units(first + p), :], stage.at[p], bsem.at[p])

    def store_wide(p):
        return pltpu.make_async_copy(stage.at[p], outs[0].at[:, units(p), :], bsem.at[p])

    def store(p, half):
        return pltpu.make_async_copy(
            obuf.at[p, :, half * SH : (half + 1) * SH, :], outs[2 * p + half], ssem.at[p, half]
        )

    if part:
        z = z_in
    else:
        z_load = pltpu.make_async_copy(z_in, z, zsem)
        z_load.start()
    for k in range(2 * pairs):
        fetch(k, k // 2).start()
    if part:
        for p in range(pairs):
            load(p).start()
    if not begin:
        acc_load = pltpu.make_async_copy(acc_in, acc, asem)
        acc_load.start()
    else:
        acc[...] = jnp.zeros_like(acc)
    router = jnp.zeros((8, PEERS * slots), F32) if begin else router_in[...]
    if not part:
        z_load.wait()

    def block(p, router):
        fetch(0, p).wait()
        fetch(1, p).wait()
        parts, dx, r = expert_block(z, slots, wbuf[p, 0], wbuf[p, 1], wbuf[p, 2])
        if part:
            load(p).wait()
            for k in range(3):
                obuf[p, k] = (parts[k] + stage[p, k]).astype(BF)
            for q in range(pairs):

                @pl.when(p == q)
                def _():
                    for half in range(2):
                        store(q, half).start()
        else:
            for k in range(3):
                stage[p, k] = parts[k]
            store_wide(p).start()
        if not begin:

            @pl.when(p == 0)
            def _():
                acc_load.wait()

        acc[...] += dx
        return router + r

    router = block(0, router) if pairs == 1 else lax.fori_loop(0, pairs, block, router)
    if end:
        rows = acc[...].astype(BF).reshape(PEERS, slots, DS)
        for g in range(slots // EXTRA):
            dbuf[:, :, g * DS : (g + 1) * DS] = rows[:, g * EXTRA : (g + 1) * EXTRA, :]
        if last:
            router_rows(dbuf, slots // EXTRA * DS, router_first[...], router)
        here = pl.ds(part * SLOTS[0] // EXTRA * DS, dbuf.shape[2])
        save = pltpu.make_async_copy(dbuf, dx_out.at[:, :, here], asem)
    else:
        save = pltpu.make_async_copy(acc, dx_out, asem)
    save.start()
    if not last:
        router_out[...] = router
    for p in range(pairs):
        if part:
            store(p, 0).wait()
            store(p, 1).wait()
        else:
            store_wide(p).wait()
    save.wait()


def expert_part(part, z, weights, before=None, at=0, carry=None, end=False, first=None):
    pairs = len(weights) // 2
    last = part == 1 and end
    slots = SLOTS[part]
    rows = PEERS * slots
    width = slots // EXTRA * DS + (128 if last else 0)
    args = [z if part else in_hbm(z), *[in_hbm(w) for w in weights]]
    in_specs = [WHOLE if part else HBM] + [HBM] * len(weights)
    if part:
        args += [in_hbm(before)]
        in_specs += [HBM]
    if carry is not None:
        args += [in_hbm(carry[0]), carry[1]]
        in_specs += [HBM, WHOLE]
    if last:
        args += [first[1], in_hbm(first[0])]
        in_specs += [WHOLE, HBM]
    if part:
        out_shape = [pltpu.HBM((3, SH, DS), BF)] * (2 * pairs)
    else:
        out_shape = [pltpu.HBM((3, pairs * UNITS, DS), F32)]
    if end:
        out_shape += [pltpu.HBM((PEERS, EXTRA, CAP // EXTRA * DS + 128), BF)]
    else:
        out_shape += [pltpu.HBM((rows, DS), F32)]
    out_specs = [HBM] * len(out_shape)
    if not last:
        out_shape += [jax.ShapeDtypeStruct((8, rows), F32)]
        out_specs += [WHOLE]
    return pl.pallas_call(
        functools.partial(
            expert_kernel, part=part, pairs=pairs, first=at, begin=carry is None, end=end
        ),
        in_specs=in_specs,
        out_specs=out_specs,
        out_shape=out_shape,
        input_output_aliases={len(args) - 1: 2 * pairs} if last else {},
        scratch_shapes=[
            pltpu.VMEM((8, 128, 128) if part else (PEERS, 2 * slots, DS), BF),
            pltpu.VMEM((rows, DS), F32),
            pltpu.VMEM((pairs, 3, UNITS, DS), BF),
            pltpu.VMEM((pairs, 3, UNITS, DS), F32),
            pltpu.VMEM((pairs, 3, UNITS, DS) if part else (8, 128), BF),
            pltpu.VMEM((PEERS, EXTRA, width) if end else (8, 128), BF),
            pltpu.SemaphoreType.DMA,
            pltpu.SemaphoreType.DMA,
            pltpu.SemaphoreType.DMA((pairs, 2)),
            pltpu.SemaphoreType.DMA((pairs,)),
            pltpu.SemaphoreType.DMA((pairs, 2)),
        ],
        compiler_params=params(36),
    )(*args)


def picks(codes, part, start, count):
    rows = PEERS * SLOTS[part]
    row = lax.broadcasted_iota(jnp.int32, (count, rows), 1) + part * PEERS * SLOTS[0]
    code0, code1 = (c[start : start + count] for c in codes)
    return jnp.where((row == code0) | (row == code1), 1.0, 0.0).astype(BF)


def columns(table):
    cols = jnp.transpose(table[...])
    whole = lambda k: cols[:, k : k + 1].astype(jnp.int32)
    return (whole(0), whole(1)), (cols[:, 2:3], cols[:, 3:4]), (whole(4), whole(5)), (whole(6), whole(7))


def slot_rows(back, part):
    slots = SLOTS[part]
    base = part * SLOTS[0] // EXTRA
    groups = [
        back[:, :, (base + g) * DS : (base + g + 1) * DS] for g in range(slots // EXTRA)
    ]
    return jnp.concatenate(groups, axis=1).reshape(PEERS * slots, DS)


def combine_kernel(table, back, out, probs):
    codes, weight, peer, slot = columns(table)
    rows = [slot_rows(back, part) for part in range(2)]
    count = 256
    n = count // 128
    for b in range(SUBS // count):
        got = contract(picks(codes, 0, b * count, count), rows[0], 1, 0)
        got = (got + contract(picks(codes, 1, b * count, count), rows[1], 1, 0)).astype(BF)
        for k in range(n):
            h = b * n + k
            out[:, h * DS : (h + 1) * DS] = got[k * 128 : (k + 1) * 128]
    at = CAP // EXTRA * DS
    routers = back[:, :, at : at + 128].reshape(PEERS * EXTRA, 128)
    source = lax.broadcasted_iota(jnp.int32, (SUBS, PEERS * EXTRA), 1)
    lane = lax.broadcasted_iota(jnp.int32, (SUBS, 128), 1)
    found = []
    for k in range(2):
        pick = jnp.where(source == peer[k] * EXTRA, 1.0, 0.0).astype(BF)
        line = contract(pick, routers, 1, 0)
        value = jnp.sum(jnp.where(lane == slot[k], line, 0.0), axis=1, keepdims=True)
        found.append(value / weight[k])
    both = jnp.where(lane == 0, found[0], jnp.where(lane == 1, found[1], 0.0))
    probs[...] = jnp.transpose(both)[0:8, :]


def combine(table, back):
    return pl.pallas_call(
        combine_kernel,
        out_shape=[
            jax.ShapeDtypeStruct((SUBS // H, H * DS), BF),
            jax.ShapeDtypeStruct((8, SUBS), F32),
        ],
        compiler_params=params(),
        name="combine",
    )(table, back)


def final_kernel(which, own0, own1, own2, own3, other, grad_in, grad_out, total, sems):
    a = which[0]

    def copies(source, at, k):
        return (
            pltpu.make_async_copy(source.at[0:2], grad_in.at[at], sems.at[k, 0]),
            pltpu.make_async_copy(source.at[2], grad_out.at[at], sems.at[k, 1]),
        )

    theirs = copies(other, 1 - a, 0)
    for c in theirs:
        c.start()
    for k in range(3):
        value = own0[k].astype(F32) + own1[k].astype(F32) + own2[k].astype(F32)
        total[k] = (value + own3[k].astype(F32)).astype(BF)
    mine = copies(total, a, 1)
    for c in mine:
        c.start()
    for c in theirs + mine:
        c.wait()


def final(which, own, other):
    return pl.pallas_call(
        final_kernel,
        in_specs=[pl.BlockSpec(memory_space=pltpu.SMEM)] + [WHOLE] * 5,
        out_specs=[HBM, HBM],
        out_shape=[pltpu.HBM((2, 2, SH, DS), BF), pltpu.HBM((2, SH, DS), BF)],
        scratch_shapes=[pltpu.VMEM((3, SH, DS), BF), pltpu.SemaphoreType.DMA((2, 2))],
        compiler_params=params(),
        name="final",
    )(which, *own, other)


def ring(a, step):
    return lax.ppermute(a, "x", [(i, (i + step) % 4) for i in range(4)])


def swap(a):
    return lax.ppermute(a, "yh", [(0, 1), (1, 0)])


def exchange(a):
    return lax.all_to_all(a, PLANE, 0, 0, tiled=True)


def add(*arrays):
    return sum(a.astype(F32) for a in arrays).astype(BF)


def layer(tokens, cotangent, expert_ids, slot_ids, route_probs, weights_in, weights_out):
    yh = lax.axis_index("yh")
    both = jnp.concatenate([weights_in, weights_out[:, None]], axis=1)
    theirs = jnp.where(yh == 0, both[1], both[0])
    w_p = swap(theirs)
    mine = lax.optimization_barrier((both, theirs))[0]
    w_o = jnp.where(yh == 0, mine[0], mine[1])
    w_o_m = ring(w_o, 1)
    w_o_p = ring(w_o, -1)
    w_p_m = ring(w_p, 1)
    w_p_p = ring(w_p, -1)
    w_o_2 = ring(w_o_p, -1)
    w_p_2 = ring(w_p_m, 1)

    dest = expert_ids % 2 * (PEERS // 2) + expert_ids // 2
    code = jnp.where(
        slot_ids < SLOTS[0],
        dest * SLOTS[0] + slot_ids,
        PEERS * SLOTS[0] + dest * SLOTS[1] + slot_ids - SLOTS[0],
    )
    table = [code, route_probs, dest, slot_ids]
    table = jnp.concatenate([t.astype(F32) for t in table], axis=2)
    table = jnp.transpose(table, (2, 1, 0)).reshape(8, SUBS)

    z1 = exchange(dispatch(table, tokens, cotangent, 0))
    z2 = exchange(dispatch(table, tokens, cotangent, 1))

    near = [w_p_p, w_p_m, w_o_p, w_o_m]
    far = [w_p_2, w_o_2]
    own = [w_p, w_o]
    dw_near, *carry = expert_part(0, z1, near)
    dw_rest, *first = expert_part(0, z1, far + own, carry=carry, end=True)
    p_2, o_2, *carry = expert_part(1, z2, far, dw_rest, 0)
    p_2 = ring(p_2, 2)
    o_2 = ring(o_2, 2)
    p_p, p_m, o_p, o_m, *carry = expert_part(1, z2, near, dw_near, 0, carry)
    p_p = ring(p_p, 1)
    p_m = ring(p_m, -1)
    o_p = ring(o_p, 1)
    o_m = ring(o_m, -1)
    p_0, o_0, back = expert_part(1, z2, own, dw_rest, 1, carry, True, first)
    back = exchange(back)
    other = swap(add(p_0, p_p, p_m, p_2))
    grad_in, grad_out = final(yh.astype(jnp.int32).reshape(1), (o_0, o_p, o_m, o_2), other)

    grad_tokens, probs = combine(table, back)
    grad_probs = jnp.transpose(probs[0:2].reshape(2, H, SUBS // H), (2, 1, 0))
    return grad_tokens, grad_probs, grad_in, grad_out


def solution(mesh):
    wide = Mesh(mesh.devices.reshape(4, 2, 4, 2, 2), AXES)
    dp = ("x", "yh")
    expert = ("z", "yl", "core")
    rows2 = P(AXES, None)
    rows3 = P(AXES, None, None)
    w_in = P(expert, None, dp, None)
    w_out = P(expert, dp, None)
    return jax.shard_map(
        layer,
        mesh=wide,
        in_specs=(rows2, rows2, rows3, rows3, rows3, w_in, w_out),
        out_specs=(rows2, rows3, w_in, w_out),
        check_vma=False,
    )
```
